512 devices in a mesh: groups: 2 (over y), shot: 32 (over z), slab: 8 (over x, core).
Axes of the slice: x: 4, y: 2, z: 32, core: 2. Of those that a mesh axis runs over, the one named last changes fastest.
The devices are a block of a 4x8x32 slice.
Arguments:
- model: float32 [128, 64, 128], P(('groups', 'slab')), parts along dimension 0, may hold values from 0.05 to 0.3
- fwd_now: float32 [64, 64, 64, 128], P(('groups', 'shot'), 'slab'), parts along dimension 0, may hold values from -6 to 6
- fwd_next: float32 [64, 64, 64, 128], P(('groups', 'shot'), 'slab'), parts along dimension 0, may hold values from -6 to 6
- adj_now: float32 [64, 64, 64, 128], P(('groups', 'shot'), 'slab'), parts along dimension 0, may hold values from -6 to 6
- adj_next: float32 [64, 64, 64, 128], P(('groups', 'shot'), 'slab'), parts along dimension 0, may hold values from -6 to 6
- wavelet: float32 [64, 8], P(('groups', 'shot')), parts along dimension 0, may hold values from -16 to 16
- misfit: float32 [64, 8, 128], P(('groups', 'shot')), parts along dimension 0, may hold values from -6 to 6
- src_index: int32 [64], P(('groups', 'shot')), parts along dimension 0, may hold values from 0 to 524287
- rec_index: int32 [64, 128], P(('groups', 'shot')), parts along dimension 0, may hold values from 0 to 524287
Outputs:
- new_model: float32 [128, 64, 128], P(('groups', 'slab')), parts along dimension 0
- stepped: float32 [64, 64, 64, 128], P(('groups', 'shot'), 'slab'), parts along dimension 0
- adjoint_start: float32 [64, 64, 64, 128], P(('groups', 'shot'), 'slab'), parts along dimension 0
The draws below stay inside these ranges and needn't reach their ends.
There are 2 independent parts, one for each index of `groups`. The reference program is written for one: setup_inputs(seed, part) draws one part's arguments, and reference() takes and returns one part's arrays. A program takes and returns all parts, laid end to end along the dimension named above; each array names one. Nothing has to cross between parts.
All inputs are finite; a program needn't handle non-finite values. Where the reference program divides by a largest or mean magnitude, that divisor is 1e-20 or more.
Results may differ from the reference program's by a relative error of at most 0.00002.
Values sent between devices are 32-bit elements; how exact they have to be, the bound alone decides.
A program may use at most 64 MiB of HBM per device.

```python
import jax
import jax.numpy as jnp

NY = 64
NZ = 128
ITERS = 8
NREC = 128
NX = 64
NSHOT = 32


def set_ends(values, key, low, top_value):
    longest = values.shape.index(max(values.shape))
    spots = []
    for shift in (0, 1):
        where = [jax.random.randint(jax.random.fold_in(key, axis), (), 0, length) for axis, length in enumerate(values.shape)]
        where[longest] = (where[longest] + shift) % values.shape[longest]
        spots.append(tuple(where))
    return values.at[spots[0]].set(low).at[spots[1]].set(top_value)


def block_scale(rng, shape, split, smallest, largest):
    def one(dim, shards_of):
        heights = jax.random.uniform(jax.random.fold_in(jax.random.fold_in(rng, 6), dim), (shards_of,), jnp.float32, smallest / len(split), largest / len(split))
        return jnp.repeat(jnp.exp(heights), shape[dim] // shards_of).reshape((-1,) + (1,) * (len(shape) - dim - 1))

    level = one(*split[0])
    for cut in split[1:]:
        level = level * one(*cut)
    return level


def normal_values(key, shape, deviation, bound, split=(), kind=jnp.bfloat16):
    values = deviation * jax.random.normal(key, shape, jnp.float32)
    if split:
        values = values * block_scale(key, shape, split, -0.22, 0.18)
    return jnp.clip(values, -bound, bound).astype(kind)


def setup_inputs(seed: int = 0, part: int = 0) -> dict:
    key_list = jax.random.split(jax.random.key(seed), 10)
    part_keys = jax.random.split(jax.random.fold_in(key_list[9], part), 10)
    return {
        "model": jnp.clip(0.05 + 0.25 * jax.random.uniform(part_keys[0], (NX, NY, NZ), jnp.float32) ** block_scale(part_keys[0], (NX, NY, NZ), ((0, 8),), -0.2, 0.2), 0.05, 0.3),
        "fwd_now": normal_values(part_keys[1], (NSHOT, NX, NY, NZ), 1.0, 6.0, ((0, 32), (1, 8)), jnp.float32),
        "fwd_next": normal_values(part_keys[2], (NSHOT, NX, NY, NZ), 1.0, 6.0, ((0, 32), (1, 8)), jnp.float32),
        "adj_now": normal_values(part_keys[3], (NSHOT, NX, NY, NZ), 1.0, 6.0, ((0, 32), (1, 8)), jnp.float32),
        "adj_next": normal_values(part_keys[4], (NSHOT, NX, NY, NZ), 1.0, 6.0, ((0, 32), (1, 8)), jnp.float32),
        "wavelet": normal_values(part_keys[5], (NSHOT, ITERS), 4.0, 16.0, ((0, 32),), jnp.float32),
        "misfit": normal_values(part_keys[6], (NSHOT, ITERS, NREC), 1.0, 6.0, ((0, 32),), jnp.float32),
        "src_index": set_ends(jax.random.randint(part_keys[7], (NSHOT,), 0, NX * NY * NZ), jax.random.fold_in(part_keys[7], 1), 0, (NX * NY * NZ) - 1).astype(jnp.int32),
        "rec_index": set_ends(jax.random.randint(part_keys[8], (NSHOT, NREC), 0, NX * NY * NZ), jax.random.fold_in(part_keys[8], 1), 0, (NX * NY * NZ) - 1).astype(jnp.int32),
    }


def laplace(field):
    padded = jnp.pad(field, ((0, 0), (1, 1), (1, 1), (1, 1)))
    beside = padded[:, 2:, 1:-1, 1:-1] + padded[:, :-2, 1:-1, 1:-1]
    beside = beside + padded[:, 1:-1, 2:, 1:-1] + padded[:, 1:-1, :-2, 1:-1]
    beside = beside + padded[:, 1:-1, 1:-1, 2:] + padded[:, 1:-1, 1:-1, :-2]
    return beside - 6.0 * field


def inject(field, index, values):
    shots = field.shape[0]
    flat = field.reshape(shots, -1)
    rows = jnp.arange(shots, dtype=jnp.int32).reshape((shots,) + (1,) * (index.ndim - 1))
    rows = jnp.broadcast_to(rows, index.shape)
    flat = flat.at[rows, index].add(values)
    return flat.reshape(field.shape)


def reference(model, fwd_now, fwd_next, adj_now, adj_next, wavelet, misfit, src_index, rec_index):
    wave, wave_later = fwd_now, fwd_next
    adjoint, adjoint_later = adj_now, adj_next
    image = jnp.zeros_like(fwd_now)
    for step in range(ITERS):
        lap_wave = laplace(wave)
        lap_adjoint = laplace(adjoint)
        image = image + adjoint * lap_wave
        wave_prior = 2.0 * wave - wave_later + model[None] * lap_wave
        wave_prior = inject(wave_prior, src_index, wavelet[:, step])
        adjoint_prior = 2.0 * adjoint - adjoint_later + model[None] * lap_adjoint
        adjoint_prior = inject(adjoint_prior, rec_index, misfit[:, step, :])
        wave_later, wave = wave, wave_prior
        adjoint_later, adjoint = adjoint, adjoint_prior
    gradient = jnp.sum(image, axis=0)
    peak = jnp.max(jnp.abs(gradient))
    new_model = jnp.clip(model - 0.1 * gradient / (peak + 1e-6), 0.05, 0.3)
    stepped = 2.0 * wave - wave_later + new_model[None] * laplace(wave)
    return new_model, stepped, adjoint
```

```python
import functools

import jax
import jax.numpy as jnp
from jax import lax
from jax.experimental import pallas as pl
from jax.experimental.pallas import tpu as pltpu
from jax.sharding import PartitionSpec as P

WINDOW = 8
PAD = 8
MESH = pl.DeviceIdType.MESH


def kernel(
    shape, iters, shots, slabs,
    wavelet, src_index, misfit_hbm, rec_hbm, model_hbm, un_hbm, ul_hbm, an_hbm, al_hbm,
    new_model_hbm, stepped_hbm, adjoint_hbm,
    now, mid, mod, lus, image, inj, src, onehot, misfit, rec,
    part, groups_sum, grad, peak_slab, peak_class, base, out_model, out_step,
    load_sem, halo_send, halo_recv, first_send, first_recv, far_sem, near_sem,
    rs_send, rs_recv, gs_send, gs_recv, ag_send, ag_recv, ps_send, ps_recv, pc_send, pc_recv, out_sem,
):
    depth, rows, cols = shape
    rounds = iters // 2
    me = lax.axis_index("shot")
    slab = lax.axis_index("slab")
    odd = lax.rem(slab, 2)
    body = pl.ds(PAD, rows)
    own = pl.ds(2, depth)

    def at_shot(offset):
        return {"shot": lax.rem(me + offset + shots, shots)}

    def at_slab(offset):
        return {"slab": lax.rem(slab + offset + slabs, slabs)}

    def signal(sem, device):
        pl.semaphore_signal(sem, inc=1, device_id=device, device_id_type=MESH)

    def remote(source, target, send, recv, device):
        return pltpu.make_async_remote_copy(
            src_ref=source, dst_ref=target, send_sem=send, recv_sem=recv, device_id=device, device_id_type=MESH
        )

    loads = [
        pltpu.make_async_copy(un_hbm.at[0], now.at[0, 0, own, body], load_sem.at[0]),
        pltpu.make_async_copy(an_hbm.at[0], now.at[0, 1, own, body], load_sem.at[1]),
        pltpu.make_async_copy(ul_hbm.at[0], mid.at[0, 0, own, body], load_sem.at[2]),
        pltpu.make_async_copy(al_hbm.at[0], mid.at[0, 1, own, body], load_sem.at[3]),
        pltpu.make_async_copy(model_hbm, mod.at[own], load_sem.at[4]),
        pltpu.make_async_copy(misfit_hbm.at[0], misfit, load_sem.at[5]),
        pltpu.make_async_copy(rec_hbm, rec, load_sem.at[6]),
    ]
    for copy in loads:
        copy.start()
    barrier = pltpu.get_barrier_semaphore()
    for offset in (1, -1):
        signal(barrier, at_slab(offset))
        signal(barrier, at_shot(offset))
    pl.semaphore_wait(barrier, 4)

    sides = (1 - odd, odd)

    def exists(side):
        return jnp.where(side == 0, slab > 0, slab < slabs - 1)

    def halo(rnd, field, side):
        return remote(
            now.at[rnd, field, pl.ds(2 + (depth - 2) * side, 2), body],
            now.at[rnd, field, pl.ds((depth + 2) * (1 - side), 2), body],
            halo_send.at[rnd, field, side], halo_recv.at[rnd, field, 1 - side],
            {"slab": slab + 2 * side - 1},
        )

    def halo_in(rnd, field, side):
        return remote(
            now.at[rnd, field, pl.ds(2 + (depth - 2) * side, 2), body],
            now.at[rnd, field, pl.ds((depth + 2) * side, 2), body],
            halo_send.at[rnd, field, side], halo_recv.at[rnd, field, side],
            {"slab": slab + 2 * side - 1},
        )

    def edge(side):
        return 2 + (depth - 1) * side

    def ghost(side):
        return 1 + (depth + 1) * side

    def first_refs(which, plane):
        if which == 2:
            return mod.at[pl.ds(plane, 1)]
        return mid.at[0, which, pl.ds(plane, 1), body]

    def first(which, side, target, arrival):
        return remote(
            first_refs(which, edge(side)), first_refs(which, ghost(target)),
            first_send.at[which, side], first_recv.at[which, arrival], {"slab": slab + 2 * side - 1},
        )

    def last(side, target, arrival):
        return remote(
            now.at[rounds, 0, pl.ds(edge(side), 1), body], now.at[rounds, 0, pl.ds(ghost(target), 1), body],
            halo_send.at[rounds, 0, side], halo_recv.at[rounds, 0, arrival], {"slab": slab + 2 * side - 1},
        )

    def on_sides(action):
        for side in sides:
            @pl.when(exists(side))
            def _():
                action(side)

    loads[0].wait()
    on_sides(lambda side: halo(0, 0, side).start())
    loads[2].wait()
    loads[4].wait()

    def send_first_u(side):
        first(0, side, 1 - side, 1 - side).start()
        first(2, side, 1 - side, 1 - side).start()

    on_sides(send_first_u)
    loads[1].wait()
    on_sides(lambda side: halo(0, 1, side).start())
    loads[3].wait()
    on_sides(lambda side: first(1, side, 1 - side, 1 - side).start())
    for offset in (1, -1):
        signal(far_sem.at[0], at_shot(offset))
        signal(near_sem.at[0], at_slab(offset))

    strip = jnp.zeros((PAD, cols), jnp.float32)
    plane0 = jnp.zeros((rows, cols), jnp.float32)

    def clear(plane, carry):
        for rnd in range(rounds + 1):
            for field in range(2):
                for ref in (now, mid):
                    ref[rnd, field, plane, 0:PAD, :] = strip
                    ref[rnd, field, plane, PAD + rows : PAD + rows + PAD, :] = strip
        image[plane] = plane0
        return carry

    lax.fori_loop(0, depth + 4, clear, 0)
    for side in range(2):
        @pl.when(jnp.logical_not(exists(side)))
        def _():
            for plane in range(2):
                at = (depth + 2) * side + plane
                mod[at] = plane0
                for field in range(2):
                    mid[0, field, at, body, :] = plane0
                    for rnd in range(rounds + 1):
                        now[rnd, field, at, body, :] = plane0

    loads[5].wait()
    loads[6].wait()
    line = lax.shift_right_logical(rec[...], 7)
    lane = jnp.bitwise_and(rec[...], cols - 1)
    src_line = lax.shift_right_logical(src_index[0], 7)
    src_lane = jnp.bitwise_and(src_index[0], cols - 1)
    row_id = lax.broadcasted_iota(jnp.int32, (rows, cols), 0)
    col_id = lax.broadcasted_iota(jnp.int32, (rows, cols), 1)

    def mark(plane, carry):
        here = row_id + (slab * depth + plane - 2) * rows
        hit = jnp.where(here == line, 1.0, 0.0).astype(jnp.bfloat16)
        at = pl.ds(pl.multiple_of(plane * rows, rows), rows)
        for copy in range(3):
            onehot[at, copy * cols : (copy + 1) * cols] = hit
        src[plane] = jnp.where((here == src_line) & (col_id == src_lane), 1.0, 0.0)
        return carry

    lax.fori_loop(1, depth + 3, mark, 0)
    cell_id = lax.broadcasted_iota(jnp.int32, (cols, cols), 0)

    def place(k, carry):
        value = jnp.where(cell_id == lane, misfit[pl.ds(k, 1), :], 0.0)
        high = value.astype(jnp.bfloat16)
        value = value - high.astype(jnp.float32)
        middle = value.astype(jnp.bfloat16)
        value = value - middle.astype(jnp.float32)
        pieces = jnp.concatenate([high, middle, value.astype(jnp.bfloat16)], axis=1)
        added = lax.dot_general(
            onehot[rows : (depth + 3) * rows, :], pieces, (((1,), (1,)), ((), ())), preferred_element_type=jnp.float32
        )
        inj[k, 1 : depth + 3] = added.reshape(depth + 2, rows, cols)
        return carry

    lax.fori_loop(0, iters, place, 0)

    first_lane = col_id == 0
    last_lane = col_id == cols - 1

    def laplace(ref, plane, center):
        left = jnp.where(first_lane, 0.0, pltpu.roll(center, 1, 1))
        right = jnp.where(last_lane, 0.0, pltpu.roll(center, cols - 1, 1))
        beside = ref[plane + 1, body, :] + ref[plane - 1, body, :]
        beside = beside + (ref[plane, PAD + 1 : PAD + 1 + rows, :] + ref[plane, PAD - 1 : PAD - 1 + rows, :])
        return beside + (left + right) - 6.0 * center

    def advance(field, state, later, target, start, count, k, slot):
        def one(index, carry):
            plane = start + index
            center = state[plane, body, :]
            lap = laplace(state, plane, center)
            fresh = 2.0 * center - later[plane, body, :] + mod[plane] * lap
            if field == 0:
                lus[slot, plane] = lap
                fresh = fresh + wavelet[0, k] * src[plane]
            else:
                image[plane] = image[plane] + center * lus[slot, plane]
                fresh = fresh + inj[k, plane]
            target[plane, body, :] = fresh
            return carry

        lax.fori_loop(0, count, one, 0)

    def both_steps(rnd, field, first_at, first_count, second_at, second_count):
        a, b, c, d = now.at[rnd, field], mid.at[rnd, field], mid.at[rnd + 1, field], now.at[rnd + 1, field]
        advance(field, a, b, c, first_at, first_count, 2 * rnd, 0)
        advance(field, c, a, d, second_at, second_count, 2 * rnd + 1, 1)

    for rnd in range(rounds):
        for field in range(2):
            if rnd == 0 and field == 0:
                pass
            both_steps(rnd, field, 3, depth - 2, 4, depth - 4)
        for side in sides:
            for field in range(2):
                @pl.when(exists(side))
                def _():
                    halo_in(rnd, field, side).wait_recv()
                    if rnd == 0:
                        first(field, side, side, side).wait_recv()
                        if field == 0:
                            first(2, side, side, side).wait_recv()

                both_steps(rnd, field, 1 + depth * side, 2, 2 + (depth - 2) * side, 2)

                @pl.when(exists(side))
                def _():
                    if rnd + 1 < rounds:
                        halo(rnd + 1, field, side).start()
                    elif field == 0:
                        last(side, 1 - side, 1 - side).start()
        if rnd < 3:
            pl.semaphore_wait(far_sem.at[rnd], 2)
            for offset in (2 << rnd, -(2 << rnd)):
                signal(far_sem.at[rnd + 1], at_shot(offset))
        if rnd < 2:
            pl.semaphore_wait(near_sem.at[rnd], 2)
        if rnd == 0:
            for offset in (2, -2):
                signal(near_sem.at[1], at_slab(offset))

    far = jnp.where(odd == 0, WINDOW // 2, -(WINDOW // 2))
    offsets = [far] + [sign * step for step in range(WINDOW // 2 - 1, 0, -1) for sign in (1, -1)]
    height = rows // WINDOW
    my_class = lax.rem(me, WINDOW)
    my_group = lax.div(me, WINDOW)
    count = shots // WINDOW

    def class_rows(which):
        return pl.ds(pl.multiple_of(which * height, height), height)

    scatter = []
    for slot, offset in enumerate(offsets):
        theirs = lax.rem(me + offset + shots, WINDOW)
        copy = remote(
            image.at[own, class_rows(theirs)], part.at[slot], rs_send.at[slot], rs_recv.at[slot], at_shot(offset)
        )
        copy.start()
        scatter.append(copy)
    adjoint_out = pltpu.make_async_copy(now.at[rounds, 1, own, body], adjoint_hbm.at[0], out_sem.at[0])
    adjoint_out.start()
    for copy in reversed(scatter):
        copy.wait_recv()

    def gather_window(plane, carry):
        total = image[plane + 2, class_rows(my_class), :]
        for slot in range(len(offsets)):
            total = total + part[slot, plane]
        groups_sum[my_group, plane] = total
        return carry

    lax.fori_loop(0, depth, gather_window, 0)
    pl.semaphore_wait(far_sem.at[3], 2)
    exchange = []
    for turn in (2, 1, 3):
        other = lax.rem(my_group + turn, count)
        copy = remote(
            groups_sum.at[my_group], groups_sum.at[my_group], gs_send.at[turn], gs_recv.at[turn], at_shot(turn * WINDOW)
        )
        copy.start()
        exchange.append((copy, other))

    def wait_last(side):
        last(side, side, side).wait_recv()

    on_sides(wait_last)

    def prepare(plane, carry):
        state = now.at[rounds, 0]
        center = state[plane, body, :]
        lus[0, plane] = laplace(state, plane, center)
        base[plane - 2] = 2.0 * center - mid[rounds, 0, plane, body, :]
        return carry

    lax.fori_loop(2, depth + 2, prepare, 0)
    for turn, (copy, other) in zip((2, 1, 3), exchange):
        origin = lax.rem(my_group + count - turn, count)
        remote(
            groups_sum.at[my_group], groups_sum.at[origin], gs_send.at[turn], gs_recv.at[turn], at_shot(turn * WINDOW)
        ).wait_recv()

    def finish(plane, carry):
        total = groups_sum[0, plane]
        for group in range(1, count):
            total = total + groups_sum[group, plane]
        grad[plane, class_rows(my_class), :] = total
        return jnp.maximum(carry, jnp.abs(total))

    top = lax.fori_loop(0, depth, finish, jnp.zeros((height, cols), jnp.float32))
    peak_slab[slab] = top
    peaks = []
    for turn in range(1, slabs):
        copy = remote(peak_slab.at[slab], peak_slab.at[slab], ps_send.at[turn], ps_recv.at[turn], at_slab(turn))
        copy.start()
        peaks.append(copy)
    gather = []
    for slot, offset in enumerate(offsets):
        mine = grad.at[:, class_rows(my_class)]
        copy = remote(mine, mine, ag_send.at[slot], ag_recv.at[slot], at_shot(offset))
        copy.start()
        gather.append(copy)
    for turn in range(1, slabs):
        origin = lax.rem(slab + slabs - turn, slabs)
        remote(
            peak_slab.at[slab], peak_slab.at[origin], ps_send.at[turn], ps_recv.at[turn], at_slab(turn)
        ).wait_recv()
    top = peak_slab[0]
    for other in range(1, slabs):
        top = jnp.maximum(top, peak_slab[other])
    peak_class[my_class] = top
    class_peaks = []
    for slot, offset in enumerate(offsets):
        copy = remote(
            peak_class.at[my_class], peak_class.at[my_class], pc_send.at[slot], pc_recv.at[slot], at_shot(offset)
        )
        copy.start()
        class_peaks.append(copy)
    for slot, offset in enumerate(offsets):
        origin = lax.rem(me - offset + shots, WINDOW)
        theirs = grad.at[:, class_rows(origin)]
        remote(theirs, theirs, ag_send.at[slot], ag_recv.at[slot], at_shot(offset)).wait_recv()
        remote(
            peak_class.at[origin], peak_class.at[origin], pc_send.at[slot], pc_recv.at[slot], at_shot(offset)
        ).wait_recv()
    top = peak_class[0]
    for other in range(1, WINDOW):
        top = jnp.maximum(top, peak_class[other])
    peak = jnp.max(jnp.max(top, axis=0, keepdims=True), axis=1, keepdims=True) + 1e-6

    def update(plane, carry):
        fresh = jnp.clip(mod[plane + 2] - 0.1 * grad[plane] / peak, 0.05, 0.3)
        out_model[plane] = fresh
        out_step[plane] = base[plane] + fresh * lus[0, plane + 2]
        return carry

    lax.fori_loop(0, depth, update, 0)
    outs = [
        pltpu.make_async_copy(out_model, new_model_hbm, out_sem.at[1]),
        pltpu.make_async_copy(out_step, stepped_hbm.at[0], out_sem.at[2]),
    ]
    for copy in outs:
        copy.start()

    def sent(side):
        for field in range(2):
            for rnd in range(rounds):
                halo(rnd, field, side).wait_send()
        last(side, 1 - side, 1 - side).wait_send()
        for which in range(3):
            first(which, side, 1 - side, 1 - side).wait_send()

    on_sides(sent)
    for copy in scatter + [pair[0] for pair in exchange] + peaks + gather + class_peaks:
        copy.wait_send()
    adjoint_out.wait()
    for copy in outs:
        copy.wait()


def solution(mesh):
    shots, slabs = mesh.shape["shot"], mesh.shape["slab"]

    def per_device(model, fwd_now, fwd_next, adj_now, adj_next, wavelet, misfit, src_index, rec_index):
        shape = model.shape
        depth, rows, cols = shape
        iters, receivers = misfit.shape[1:]
        rounds = iters // 2
        f32 = jnp.float32
        dma = pltpu.SemaphoreType.DMA
        height = rows // WINDOW
        smem = pl.BlockSpec(memory_space=pltpu.SMEM)
        hbm = pl.BlockSpec(memory_space=pl.ANY)
        return pl.pallas_call(
            functools.partial(kernel, shape, iters, shots, slabs),
            out_shape=(
                jax.ShapeDtypeStruct(shape, f32),
                jax.ShapeDtypeStruct(fwd_now.shape, f32),
                jax.ShapeDtypeStruct(adj_now.shape, f32),
            ),
            in_specs=[smem, smem] + [hbm] * 7,
            out_specs=(hbm, hbm, hbm),
            scratch_shapes=[
                pltpu.VMEM((rounds + 1, 2, depth + 4, rows + 2 * PAD, cols), f32),
                pltpu.VMEM((rounds + 1, 2, depth + 4, rows + 2 * PAD, cols), f32),
                pltpu.VMEM((depth + 4, rows, cols), f32),
                pltpu.VMEM((2, depth + 4, rows, cols), f32),
                pltpu.VMEM((depth + 4, rows, cols), f32),
                pltpu.VMEM((iters, depth + 4, rows, cols), f32),
                pltpu.VMEM((depth + 4, rows, cols), f32),
                pltpu.VMEM(((depth + 4) * rows, 3 * receivers), jnp.bfloat16),
                pltpu.VMEM((iters, receivers), f32),
                pltpu.VMEM((1, receivers), jnp.int32),
                pltpu.VMEM((WINDOW - 1, depth, height, cols), f32),
                pltpu.VMEM((shots // WINDOW, depth, height, cols), f32),
                pltpu.VMEM(shape, f32),
                pltpu.VMEM((slabs, height, cols), f32),
                pltpu.VMEM((WINDOW, height, cols), f32),
                pltpu.VMEM(shape, f32),
                pltpu.VMEM(shape, f32),
                pltpu.VMEM(shape, f32),
                dma((7,)),
                dma((rounds + 1, 2, 2)), dma((rounds + 1, 2, 2)),
                dma((3, 2)), dma((3, 2)),
                pltpu.SemaphoreType.REGULAR((4,)), pltpu.SemaphoreType.REGULAR((2,)),
                dma((WINDOW - 1,)), dma((WINDOW - 1,)),
                dma((shots // WINDOW,)), dma((shots // WINDOW,)),
                dma((WINDOW - 1,)), dma((WINDOW - 1,)),
                dma((slabs,)), dma((slabs,)),
                dma((WINDOW - 1,)), dma((WINDOW - 1,)),
                dma((3,)),
            ],
            compiler_params=pltpu.CompilerParams(
                collective_id=0, has_side_effects=True, vmem_limit_bytes=48 * 1024 * 1024
            ),
            name="reverse_time",
        )(wavelet, src_index, misfit, rec_index, model, fwd_now, fwd_next, adj_now, adj_next)

    field = P(("groups", "shot"), "slab", None, None)
    model_spec = P(("groups", "slab"), None, None)
    return jax.shard_map(
        per_device,
        mesh=mesh,
        in_specs=(
            model_spec, field, field, field, field,
            P(("groups", "shot"), None), P(("groups", "shot"), None, None), P(("groups", "shot")),
            P(("groups", "shot"), None),
        ),
        out_specs=(model_spec, field, field),
        check_vma=False,
    )
```

```python
import functools

import jax
import jax.numpy as jnp
from jax import lax
from jax.experimental import pallas as pl
from jax.experimental.pallas import tpu as pltpu
from jax.sharding import PartitionSpec as P

WINDOW = 8
PAD = 8
MESH = pl.DeviceIdType.MESH


def kernel(
    shape, iters, shots, slabs,
    src_index, wavelet_hbm, misfit_hbm, rec_hbm, model_hbm, un_hbm, ul_hbm, an_hbm, al_hbm,
    grad_out, peak_out, model_out, base_out, lap_out, adjoint_out,
    now, mid, mod, lus, image, inj, src, onehot, misfit, rec, wavelet,
    part, groups_sum, grad, peak_slab, peak_class,
    load_sem, halo_send, halo_recv, first_send, first_recv, far_sem, near_sem,
    rs_send, rs_recv, gs_send, gs_recv, relay_send, relay_recv, ag_send, ag_recv, ps_send, ps_recv, pc_send, pc_recv,
):
    depth, rows, cols = shape
    rounds = iters // 2
    me = lax.axis_index("shot")
    slab = lax.axis_index("slab")
    odd = lax.rem(slab, 2)
    body = pl.ds(PAD, rows)
    own = pl.ds(2, depth)

    def at_shot(offset):
        return {"shot": lax.rem(me + offset + shots, shots)}

    def at_slab(offset):
        return {"slab": lax.rem(slab + offset + slabs, slabs)}

    def signal(sem, device):
        pl.semaphore_signal(sem, inc=1, device_id=device, device_id_type=MESH)

    def remote(source, target, send, recv, device):
        return pltpu.make_async_remote_copy(
            src_ref=source, dst_ref=target, send_sem=send, recv_sem=recv, device_id=device, device_id_type=MESH
        )

    loads = [
        pltpu.make_async_copy(un_hbm.at[0], now.at[0, 0, own, body], load_sem.at[0]),
        pltpu.make_async_copy(an_hbm.at[0], now.at[0, 1, own, body], load_sem.at[1]),
        pltpu.make_async_copy(ul_hbm.at[0], mid.at[0, 0, own, body], load_sem.at[2]),
        pltpu.make_async_copy(al_hbm.at[0], mid.at[0, 1, own, body], load_sem.at[3]),
        pltpu.make_async_copy(model_hbm, mod.at[own], load_sem.at[4]),
        pltpu.make_async_copy(misfit_hbm.at[0], misfit, load_sem.at[5]),
        pltpu.make_async_copy(rec_hbm, rec, load_sem.at[6]),
        pltpu.make_async_copy(wavelet_hbm, wavelet, load_sem.at[7]),
    ]
    for copy in loads:
        copy.start()
    barrier = pltpu.get_barrier_semaphore()
    for offset in (1, -1):
        signal(barrier, at_slab(offset))
        signal(barrier, at_shot(offset))
    pl.semaphore_wait(barrier, 4)

    sides = (1 - odd, odd)

    def exists(side):
        return jnp.where(side == 0, slab > 0, slab < slabs - 1)

    def halo(rnd, field, side):
        return remote(
            now.at[rnd, field, pl.ds(2 + (depth - 2) * side, 2), body],
            now.at[rnd, field, pl.ds((depth + 2) * (1 - side), 2), body],
            halo_send.at[rnd, field, side], halo_recv.at[rnd, field, 1 - side],
            {"slab": slab + 2 * side - 1},
        )

    def halo_in(rnd, field, side):
        return remote(
            now.at[rnd, field, pl.ds(2 + (depth - 2) * side, 2), body],
            now.at[rnd, field, pl.ds((depth + 2) * side, 2), body],
            halo_send.at[rnd, field, side], halo_recv.at[rnd, field, side],
            {"slab": slab + 2 * side - 1},
        )

    def edge(side):
        return 2 + (depth - 1) * side

    def ghost(side):
        return 1 + (depth + 1) * side

    def first_refs(which, plane):
        if which == 2:
            return mod.at[pl.ds(plane, 1)]
        return mid.at[0, which, pl.ds(plane, 1), body]

    def first(which, side, target, arrival):
        return remote(
            first_refs(which, edge(side)), first_refs(which, ghost(target)),
            first_send.at[which, side], first_recv.at[which, arrival], {"slab": slab + 2 * side - 1},
        )

    def last(side, target, arrival):
        return remote(
            now.at[rounds, 0, pl.ds(edge(side), 1), body], now.at[rounds, 0, pl.ds(ghost(target), 1), body],
            halo_send.at[rounds, 0, side], halo_recv.at[rounds, 0, arrival], {"slab": slab + 2 * side - 1},
        )

    def on_sides(action):
        for side in sides:
            @pl.when(exists(side))
            def _():
                action(side)

    loads[0].wait()
    on_sides(lambda side: halo(0, 0, side).start())
    loads[2].wait()
    loads[4].wait()

    def send_first_u(side):
        first(0, side, 1 - side, 1 - side).start()
        first(2, side, 1 - side, 1 - side).start()

    on_sides(send_first_u)
    loads[1].wait()
    on_sides(lambda side: halo(0, 1, side).start())
    loads[3].wait()
    on_sides(lambda side: first(1, side, 1 - side, 1 - side).start())
    for offset in (1, -1):
        signal(far_sem.at[0], at_shot(offset))
        signal(near_sem.at[0], at_slab(offset))

    strip = jnp.zeros((PAD, cols), jnp.float32)
    plane0 = jnp.zeros((rows, cols), jnp.float32)

    def clear(plane, carry):
        for rnd in range(rounds + 1):
            for field in range(2):
                for ref in (now, mid):
                    ref[rnd, field, plane, 0:PAD, :] = strip
                    ref[rnd, field, plane, PAD + rows : PAD + rows + PAD, :] = strip
        image[plane] = plane0
        return carry

    lax.fori_loop(0, depth + 4, clear, 0)
    for side in range(2):
        @pl.when(jnp.logical_not(exists(side)))
        def _():
            for plane in range(2):
                at = (depth + 2) * side + plane
                mod[at] = plane0
                for field in range(2):
                    mid[0, field, at, body, :] = plane0
                    for rnd in range(rounds + 1):
                        now[rnd, field, at, body, :] = plane0

    for copy in loads[5:]:
        copy.wait()
    line = lax.shift_right_logical(rec[...], 7)
    lane = jnp.bitwise_and(rec[...], cols - 1)
    src_line = lax.shift_right_logical(src_index[0], 7)
    src_lane = jnp.bitwise_and(src_index[0], cols - 1)
    row_id = lax.broadcasted_iota(jnp.int32, (rows, cols), 0)
    col_id = lax.broadcasted_iota(jnp.int32, (rows, cols), 1)

    def mark(plane, carry):
        here = row_id + (slab * depth + plane - 2) * rows
        hit = jnp.where(here == line, 1.0, 0.0).astype(jnp.bfloat16)
        at = pl.ds(pl.multiple_of(plane * rows, rows), rows)
        for copy in range(3):
            onehot[at, copy * cols : (copy + 1) * cols] = hit
        src[plane] = jnp.where((here == src_line) & (col_id == src_lane), 1.0, 0.0)
        return carry

    lax.fori_loop(1, depth + 3, mark, 0)
    cell_id = lax.broadcasted_iota(jnp.int32, (cols, cols), 0)

    def place(k, carry):
        value = jnp.where(cell_id == lane, misfit[pl.ds(k, 1), :], 0.0)
        high = value.astype(jnp.bfloat16)
        value = value - high.astype(jnp.float32)
        middle = value.astype(jnp.bfloat16)
        value = value - middle.astype(jnp.float32)
        pieces = jnp.concatenate([high, middle, value.astype(jnp.bfloat16)], axis=1)
        added = lax.dot_general(
            onehot[rows : (depth + 3) * rows, :], pieces, (((1,), (1,)), ((), ())), preferred_element_type=jnp.float32
        )
        inj[k, 1 : depth + 3] = added.reshape(depth + 2, rows, cols)
        return carry

    lax.fori_loop(0, iters, place, 0)

    first_lane = col_id == 0
    last_lane = col_id == cols - 1

    def laplace(ref, plane, center):
        left = jnp.where(first_lane, 0.0, pltpu.roll(center, 1, 1))
        right = jnp.where(last_lane, 0.0, pltpu.roll(center, cols - 1, 1))
        beside = ref[plane + 1, body, :] + ref[plane - 1, body, :]
        beside = beside + (ref[plane, PAD + 1 : PAD + 1 + rows, :] + ref[plane, PAD - 1 : PAD - 1 + rows, :])
        return beside + (left + right) - 6.0 * center

    def advance(field, state, later, target, start, count, k, slot):
        def one(index, carry):
            plane = start + index
            center = state[plane, body, :]
            lap = laplace(state, plane, center)
            fresh = 2.0 * center - later[plane, body, :] + mod[plane] * lap
            if field == 0:
                lus[slot, plane] = lap
                fresh = fresh + wavelet[0, k] * src[plane]
            else:
                image[plane] = image[plane] + center * lus[slot, plane]
                fresh = fresh + inj[k, plane]
            target[plane, body, :] = fresh
            return carry

        lax.fori_loop(0, count, one, 0)

    def both_steps(rnd, field, first_at, first_count, second_at, second_count):
        a, b, c, d = now.at[rnd, field], mid.at[rnd, field], mid.at[rnd + 1, field], now.at[rnd + 1, field]
        advance(field, a, b, c, first_at, first_count, 2 * rnd, 0)
        advance(field, c, a, d, second_at, second_count, 2 * rnd + 1, 1)

    far = jnp.where(odd == 0, WINDOW // 2, -(WINDOW // 2))
    offsets = [far] + [sign * step for step in range(WINDOW // 2 - 1, 0, -1) for sign in (1, -1)]
    height = rows // WINDOW
    my_class = lax.rem(me, WINDOW)
    my_group = lax.div(me, WINDOW)
    count = shots // WINDOW
    half = depth // 2
    sends = []

    def class_rows(which):
        return pl.ds(pl.multiple_of(which * height, height), height)

    def scatter(piece, source, length, target):
        copies = []
        for slot, offset in enumerate(offsets):
            theirs = lax.rem(me + offset + shots, WINDOW)
            copy = remote(
                image.at[pl.ds(source, length), class_rows(theirs)], part.at[slot, pl.ds(target, length)],
                rs_send.at[piece, slot], rs_recv.at[piece, slot], at_shot(offset),
            )
            copy.start()
            copies.append(copy)
        sends.extend(copies)
        return copies

    scattered = [[], []]
    for rnd in range(rounds):
        for field in range(2):
            both_steps(rnd, field, 3, depth - 2, 4, depth - 4)
        if rnd + 1 == rounds:
            scattered[0] += scatter(0, 4, half, 0)
        for side in sides:
            for field in range(2):
                @pl.when(exists(side))
                def _():
                    halo_in(rnd, field, side).wait_recv()
                    if rnd == 0:
                        first(field, side, side, side).wait_recv()
                        if field == 0:
                            first(2, side, side, side).wait_recv()

                both_steps(rnd, field, 1 + depth * side, 2, 2 + (depth - 2) * side, 2)

                if rnd + 1 == rounds and field == 1:
                    scattered[1] += scatter(1 + side, 2 + (depth - 2) * side, 2, half + 2 * side)

                @pl.when(exists(side))
                def _():
                    if rnd + 1 < rounds:
                        halo(rnd + 1, field, side).start()
                    elif field == 0:
                        last(side, 1 - side, 1 - side).start()
        if rnd < 3:
            pl.semaphore_wait(far_sem.at[rnd], 2)
        if rnd < 2:
            for offset in (2 << rnd, -(2 << rnd)):
                signal(far_sem.at[rnd + 1], at_shot(offset))
            pl.semaphore_wait(near_sem.at[rnd], 2)
        if rnd == 0:
            for offset in (2, -2):
                signal(near_sem.at[1], at_slab(offset))

    def at_group(turn):
        return lax.rem(my_group + turn + count, count)

    def passed(piece, turn):
        start = half * piece
        mine = groups_sum.at[my_group, pl.ds(start, half)]
        return remote(
            mine, mine, gs_send.at[piece, turn], gs_recv.at[piece, turn], at_shot(WINDOW if turn else -WINDOW)
        )

    def passed_in(piece, turn):
        start = half * piece
        origin = at_group(-1 if turn else 1)
        theirs = groups_sum.at[origin, pl.ds(start, half)]
        return remote(
            theirs, theirs, gs_send.at[piece, turn], gs_recv.at[piece, turn], at_shot(WINDOW if turn else -WINDOW)
        )

    def relayed(piece, turn, origin):
        start = half * piece + (half // 2) * (1 - turn)
        theirs = groups_sum.at[origin, pl.ds(start, half // 2)]
        return remote(
            theirs, theirs, relay_send.at[piece, turn], relay_recv.at[piece, turn], at_shot(WINDOW if turn else -WINDOW)
        )

    for piece in range(2):
        for copy in scattered[piece]:
            copy.wait_recv()
        for slot in range(half * piece, half * (piece + 1)):
            plane = slot + 4 if piece == 0 else (slot - half + 2 if slot < half + 2 else slot + 2)
            total = image[plane, class_rows(my_class), :]
            for index in range(len(offsets)):
                total = total + part[index, slot]
            groups_sum[my_group, slot] = total
        for turn in range(2):
            copy = passed(piece, turn)
            copy.start()
            sends.append(copy)

    on_sides(lambda side: last(side, side, side).wait_recv())

    def prepare(plane, carry):
        state = now.at[rounds, 0]
        center = state[plane, body, :]
        lap_out[plane - 2] = laplace(state, plane, center)
        base_out[plane - 2] = 2.0 * center - mid[rounds, 0, plane, body, :]
        adjoint_out[plane - 2] = now[rounds, 1, plane, body, :]
        model_out[plane - 2] = mod[plane]
        return carry

    lax.fori_loop(2, depth + 2, prepare, 0)
    for piece in range(2):
        for turn in range(2):
            passed_in(piece, turn).wait_recv()
            copy = relayed(piece, turn, at_group(-1 if turn else 1))
            copy.start()
            sends.append(copy)

    top = jnp.zeros((height, cols), jnp.float32)
    for piece in range(2):
        for turn in range(2):
            relayed(piece, turn, at_group(2)).wait_recv()
        for slot in range(half * piece, half * (piece + 1)):
            total = groups_sum[0, slot]
            for group in range(1, count):
                total = total + groups_sum[group, slot]
            grad[slot, class_rows(my_class), :] = total
            top = jnp.maximum(top, jnp.abs(total))
        if piece == 1:
            peak_slab[slab] = top
            for turn in range(1, slabs):
                copy = remote(peak_slab.at[slab], peak_slab.at[slab], ps_send.at[turn], ps_recv.at[turn], at_slab(turn))
                copy.start()
                sends.append(copy)
        for slot, offset in enumerate(offsets):
            mine = grad.at[pl.ds(half * piece, half), class_rows(my_class)]
            copy = remote(mine, mine, ag_send.at[piece, slot], ag_recv.at[piece, slot], at_shot(offset))
            copy.start()
            sends.append(copy)
    for turn in range(1, slabs):
        theirs = peak_slab.at[lax.rem(slab + slabs - turn, slabs)]
        remote(theirs, theirs, ps_send.at[turn], ps_recv.at[turn], at_slab(turn)).wait_recv()
    top = peak_slab[0]
    for other in range(1, slabs):
        top = jnp.maximum(top, peak_slab[other])
    peak_class[my_class] = top
    for slot, offset in enumerate(offsets):
        mine = peak_class.at[my_class]
        copy = remote(mine, mine, pc_send.at[slot], pc_recv.at[slot], at_shot(offset))
        copy.start()
        sends.append(copy)
    for piece in range(2):
        for slot, offset in enumerate(offsets):
            theirs = grad.at[pl.ds(half * piece, half), class_rows(lax.rem(me - offset + shots, WINDOW))]
            remote(theirs, theirs, ag_send.at[piece, slot], ag_recv.at[piece, slot], at_shot(offset)).wait_recv()
        for slot in range(half * piece, half * (piece + 1)):
            grad_out[slot] = grad[slot]
    for slot, offset in enumerate(offsets):
        theirs = peak_class.at[lax.rem(me - offset + shots, WINDOW)]
        remote(theirs, theirs, pc_send.at[slot], pc_recv.at[slot], at_shot(offset)).wait_recv()
    top = peak_class[0]
    for other in range(1, WINDOW):
        top = jnp.maximum(top, peak_class[other])
    peak_out[...] = top

    def sent(side):
        for field in range(2):
            for rnd in range(rounds):
                halo(rnd, field, side).wait_send()
        last(side, 1 - side, 1 - side).wait_send()
        for which in range(3):
            first(which, side, 1 - side, 1 - side).wait_send()

    on_sides(sent)
    for copy in sends:
        copy.wait_send()


def update(shape, grad, top, model, base, lap, adjoint, new_model_hbm, stepped_hbm, adjoint_hbm, fresh_all, step_all, sem):
    depth = shape[0]
    half = depth // 2
    kept = pltpu.make_async_copy(adjoint, adjoint_hbm.at[0], sem.at[0])
    kept.start()
    peak = jnp.max(jnp.max(top[...], axis=0, keepdims=True), axis=1, keepdims=True) + 1e-6
    copies = [kept]
    for slot in range(depth):
        plane = slot + 2 if slot < half else (slot - half if slot < half + 2 else slot)
        fresh = jnp.clip(model[plane] - 0.1 * grad[slot] / peak, 0.05, 0.3)
        fresh_all[plane] = fresh
        step_all[plane] = base[plane] + fresh * lap[plane]
        if slot == half - 1:
            planes = pl.ds(2, half)
        elif slot == half + 1:
            planes = pl.ds(0, 2)
        elif slot == depth - 1:
            planes = pl.ds(depth - 2, 2)
        else:
            continue
        for source, target in ((fresh_all, new_model_hbm), (step_all, stepped_hbm.at[0])):
            copy = pltpu.make_async_copy(source.at[planes], target.at[planes], sem.at[len(copies)])
            copy.start()
            copies.append(copy)
    for copy in copies:
        copy.wait()


def solution(mesh):
    shots, slabs = mesh.shape["shot"], mesh.shape["slab"]

    def per_device(model, fwd_now, fwd_next, adj_now, adj_next, wavelet, misfit, src_index, rec_index):
        shape = model.shape
        depth, rows, cols = shape
        iters, receivers = misfit.shape[1:]
        rounds = iters // 2
        f32 = jnp.float32
        dma = pltpu.SemaphoreType.DMA
        height = rows // WINDOW
        hbm = pl.BlockSpec(memory_space=pl.ANY)
        vmem = pl.BlockSpec(memory_space=pltpu.VMEM)
        whole = jax.ShapeDtypeStruct(shape, f32)
        arguments = (wavelet, misfit, rec_index, model, fwd_now, fwd_next, adj_now, adj_next)
        results = pl.pallas_call(
            functools.partial(kernel, shape, iters, shots, slabs),
            out_shape=(whole, jax.ShapeDtypeStruct((height, cols), f32), whole, whole, whole, whole),
            in_specs=[pl.BlockSpec(memory_space=pltpu.SMEM)] + [hbm] * 8,
            out_specs=(vmem,) * 6,
            scratch_shapes=[
                pltpu.VMEM((rounds + 1, 2, depth + 4, rows + 2 * PAD, cols), f32),
                pltpu.VMEM((rounds + 1, 2, depth + 4, rows + 2 * PAD, cols), f32),
                pltpu.VMEM((depth + 4, rows, cols), f32),
                pltpu.VMEM((2, depth + 4, rows, cols), f32),
                pltpu.VMEM((depth + 4, rows, cols), f32),
                pltpu.VMEM((iters, depth + 4, rows, cols), f32),
                pltpu.VMEM((depth + 4, rows, cols), f32),
                pltpu.VMEM(((depth + 4) * rows, 3 * receivers), jnp.bfloat16),
                pltpu.VMEM((iters, receivers), f32),
                pltpu.VMEM((1, receivers), jnp.int32),
                pltpu.SMEM((1, iters), f32),
                pltpu.VMEM((WINDOW - 1, depth, height, cols), f32),
                pltpu.VMEM((shots // WINDOW, depth, height, cols), f32),
                pltpu.VMEM(shape, f32),
                pltpu.VMEM((slabs, height, cols), f32),
                pltpu.VMEM((WINDOW, height, cols), f32),
                dma((8,)),
                dma((rounds + 1, 2, 2)), dma((rounds + 1, 2, 2)),
                dma((3, 2)), dma((3, 2)),
                pltpu.SemaphoreType.REGULAR((3,)), pltpu.SemaphoreType.REGULAR((2,)),
                dma((3, WINDOW - 1)), dma((3, WINDOW - 1)),
                dma((2, 2)), dma((2, 2)),
                dma((2, 2)), dma((2, 2)),
                dma((2, WINDOW - 1)), dma((2, WINDOW - 1)),
                dma((slabs,)), dma((slabs,)),
                dma((WINDOW - 1,)), dma((WINDOW - 1,)),
            ],
            compiler_params=pltpu.CompilerParams(
                collective_id=0, has_side_effects=True, vmem_limit_bytes=48 * 1024 * 1024
            ),
            name="reverse_time",
        )(src_index, *(pltpu.with_memory_space_constraint(value, pltpu.HBM) for value in arguments))
        return pl.pallas_call(
            functools.partial(update, shape),
            out_shape=(
                whole, jax.ShapeDtypeStruct(fwd_now.shape, f32), jax.ShapeDtypeStruct(adj_now.shape, f32)
            ),
            in_specs=[vmem] * 6,
            out_specs=(hbm,) * 3,
            scratch_shapes=[pltpu.VMEM(shape, f32), pltpu.VMEM(shape, f32), dma((7,))],
            compiler_params=pltpu.CompilerParams(vmem_limit_bytes=8 * 1024 * 1024),
            name="model_update",
        )(*results)

    field = P(("groups", "shot"), "slab", None, None)
    model_spec = P(("groups", "slab"), None, None)
    return jax.shard_map(
        per_device,
        mesh=mesh,
        in_specs=(
            model_spec, field, field, field, field,
            P(("groups", "shot"), None), P(("groups", "shot"), None, None), P(("groups", "shot")),
            P(("groups", "shot"), None),
        ),
        out_specs=(model_spec, field, field),
        check_vma=False,
    )
```

```python
import functools

import jax
import jax.numpy as jnp
from jax import lax
from jax.experimental import pallas as pl
from jax.experimental.pallas import tpu as pltpu
from jax.sharding import PartitionSpec as P

WINDOW = 8
PAD = 8
MESH = pl.DeviceIdType.MESH


def kernel(
    shape, iters, shots, slabs,
    src_index, wavelet_hbm, misfit_hbm, rec_hbm, model_hbm, un_hbm, ul_hbm, an_hbm, al_hbm,
    grad_out, peak_out, model_out, base_out, lap_out, adjoint_out,
    now, mid, mod, lus, image, inj, src, onehot, misfit, rec, wavelet,
    part, groups_sum, grad, tops,
    load_sem, halo_send, halo_recv, far_sem, near_sem, sum_send, rs_recv, gs_recv, relay_recv, ag_recv, top_recv,
):
    depth, rows, cols = shape
    rounds = iters // 2
    me = lax.axis_index("shot")
    slab = lax.axis_index("slab")
    odd = lax.rem(slab, 2)
    body = pl.ds(PAD, rows)
    own = pl.ds(2, depth)

    def at_shot(offset):
        return {"shot": lax.rem(me + offset + shots, shots)}

    def at_slab(offset):
        return {"slab": lax.rem(slab + offset + slabs, slabs)}

    def signal(sem, device):
        pl.semaphore_signal(sem, inc=1, device_id=device, device_id_type=MESH)

    def remote(source, target, send, recv, device):
        return pltpu.make_async_remote_copy(
            src_ref=source, dst_ref=target, send_sem=send, recv_sem=recv, device_id=device, device_id_type=MESH
        )

    def absorb(ref, sem):
        pltpu.make_async_copy(ref, ref, sem).wait()

    loads = [
        pltpu.make_async_copy(un_hbm.at[0], now.at[0, 0, own, body], load_sem.at[0]),
        pltpu.make_async_copy(ul_hbm.at[0], mid.at[0, 0, own, body], load_sem.at[0]),
        pltpu.make_async_copy(model_hbm, mod.at[own], load_sem.at[0]),
        pltpu.make_async_copy(an_hbm.at[0], now.at[0, 1, own, body], load_sem.at[1]),
        pltpu.make_async_copy(al_hbm.at[0], mid.at[0, 1, own, body], load_sem.at[1]),
        pltpu.make_async_copy(misfit_hbm.at[0], misfit, load_sem.at[2]),
        pltpu.make_async_copy(rec_hbm, rec, load_sem.at[3]),
        pltpu.make_async_copy(wavelet_hbm, wavelet, load_sem.at[4]),
    ]
    for copy in loads:
        copy.start()
    barrier = pltpu.get_barrier_semaphore()
    for offset in (1, -1):
        signal(barrier, at_slab(offset))
        signal(barrier, at_shot(offset))
    pl.semaphore_wait(barrier, 4)

    sides = (1 - odd, odd)

    def exists(side):
        return jnp.where(side == 0, slab > 0, slab < slabs - 1)

    def send(side, source, target, rnd, field):
        remote(
            source, target, halo_send.at[side], halo_recv.at[rnd % 2, field, 1 - side], {"slab": slab + 2 * side - 1}
        ).start()

    def send_halo(rnd, field, side):
        send(
            side,
            now.at[rnd, field, pl.ds(2 + (depth - 2) * side, 2), body],
            now.at[rnd, field, pl.ds((depth + 2) * (1 - side), 2), body],
            rnd, field,
        )

    def edge(side):
        return pl.ds(2 + (depth - 1) * side, 1)

    def ghost(side):
        return pl.ds(1 + (depth + 1) * side, 1)

    def arrived(planes, rnd, field, side):
        absorb(inj.at[0, pl.ds(0, planes)], halo_recv.at[rnd % 2, field, side])

    def on_sides(action):
        for side in sides:
            @pl.when(exists(side))
            def _():
                action(side)

    def first_u(side):
        send_halo(0, 0, side)
        send(side, mid.at[0, 0, edge(side), body], mid.at[0, 0, ghost(1 - side), body], 0, 0)
        send(side, mod.at[edge(side)], mod.at[ghost(1 - side)], 0, 0)

    def first_a(side):
        send_halo(0, 1, side)
        send(side, mid.at[0, 1, edge(side), body], mid.at[0, 1, ghost(1 - side), body], 0, 1)

    def last_u(side):
        send(side, now.at[rounds, 0, edge(side), body], now.at[rounds, 0, ghost(1 - side), body], rounds, 0)

    absorb(inj.at[0:2, 0 : depth + 4], load_sem.at[0])
    on_sides(first_u)
    absorb(inj.at[0:2, 0:depth], load_sem.at[1])
    on_sides(first_a)
    for offset in (1, -1):
        signal(far_sem.at[0], at_shot(offset))
        signal(near_sem.at[0], at_slab(offset))

    strip = jnp.zeros((PAD, cols), jnp.float32)
    plane0 = jnp.zeros((rows, cols), jnp.float32)

    def clear(plane, carry):
        for rnd in range(rounds + 1):
            for field in range(2):
                for ref in (now, mid):
                    ref[rnd, field, plane, 0:PAD, :] = strip
                    ref[rnd, field, plane, PAD + rows : PAD + rows + PAD, :] = strip
        image[plane] = plane0
        return carry

    lax.fori_loop(0, depth + 4, clear, 0)
    for side in range(2):
        @pl.when(jnp.logical_not(exists(side)))
        def _():
            for plane in range(2):
                at = (depth + 2) * side + plane
                mod[at] = plane0
                for field in range(2):
                    mid[0, field, at, body, :] = plane0
                    for rnd in range(rounds + 1):
                        now[rnd, field, at, body, :] = plane0

    for copy in loads[-3:]:
        copy.wait()
    line = lax.shift_right_logical(rec[...], 7)
    lane = jnp.bitwise_and(rec[...], cols - 1)
    src_line = lax.shift_right_logical(src_index[0], 7)
    src_lane = jnp.bitwise_and(src_index[0], cols - 1)
    row_id = lax.broadcasted_iota(jnp.int32, (rows, cols), 0)
    col_id = lax.broadcasted_iota(jnp.int32, (rows, cols), 1)

    def mark(plane, carry):
        here = row_id + (slab * depth + plane - 2) * rows
        hit = jnp.where(here == line, 1.0, 0.0).astype(jnp.bfloat16)
        at = pl.ds(pl.multiple_of(plane * rows, rows), rows)
        for copy in range(3):
            onehot[at, copy * cols : (copy + 1) * cols] = hit
        src[plane] = jnp.where((here == src_line) & (col_id == src_lane), 1.0, 0.0)
        return carry

    lax.fori_loop(1, depth + 3, mark, 0)
    cell_id = lax.broadcasted_iota(jnp.int32, (cols, cols), 0)

    def place(k, carry):
        value = jnp.where(cell_id == lane, misfit[pl.ds(k, 1), :], 0.0)
        high = value.astype(jnp.bfloat16)
        value = value - high.astype(jnp.float32)
        middle = value.astype(jnp.bfloat16)
        value = value - middle.astype(jnp.float32)
        pieces = jnp.concatenate([high, middle, value.astype(jnp.bfloat16)], axis=1)
        added = lax.dot_general(
            onehot[rows : (depth + 3) * rows, :], pieces, (((1,), (1,)), ((), ())), preferred_element_type=jnp.float32
        )
        inj[k, 1 : depth + 3] = added.reshape(depth + 2, rows, cols)
        return carry

    lax.fori_loop(0, iters, place, 0)

    first_lane = col_id == 0
    last_lane = col_id == cols - 1

    def laplace(ref, plane, center):
        left = jnp.where(first_lane, 0.0, pltpu.roll(center, 1, 1))
        right = jnp.where(last_lane, 0.0, pltpu.roll(center, cols - 1, 1))
        beside = ref[plane + 1, body, :] + ref[plane - 1, body, :]
        beside = beside + (ref[plane, PAD + 1 : PAD + 1 + rows, :] + ref[plane, PAD - 1 : PAD - 1 + rows, :])
        return beside + (left + right) - 6.0 * center

    def advance(field, state, later, target, start, count, k, slot):
        def one(index, carry):
            plane = start + index
            center = state[plane, body, :]
            lap = laplace(state, plane, center)
            fresh = 2.0 * center - later[plane, body, :] + mod[plane] * lap
            if field == 0:
                lus[slot, plane] = lap
                fresh = fresh + wavelet[0, k] * src[plane]
            else:
                image[plane] = image[plane] + center * lus[slot, plane]
                fresh = fresh + inj[k, plane]
            target[plane, body, :] = fresh
            return carry

        lax.fori_loop(0, count, one, 0)

    def both_steps(rnd, field, first_at, first_count, second_at, second_count):
        a, b, c, d = now.at[rnd, field], mid.at[rnd, field], mid.at[rnd + 1, field], now.at[rnd + 1, field]
        advance(field, a, b, c, first_at, first_count, 2 * rnd, 0)
        advance(field, c, a, d, second_at, second_count, 2 * rnd + 1, 1)

    far = jnp.where(odd == 0, WINDOW // 2, -(WINDOW // 2))
    offsets = [far] + [sign * step for step in range(WINDOW // 2 - 1, 0, -1) for sign in (1, -1)]
    height = rows // WINDOW
    my_class = lax.rem(me, WINDOW)
    my_group = lax.div(me, WINDOW)
    count = shots // WINDOW
    half = depth // 2

    def class_rows(which):
        return pl.ds(pl.multiple_of(which * height, height), height)

    def scatter(piece, source, length, target):
        for slot, offset in enumerate(offsets):
            theirs = lax.rem(me + offset + shots, WINDOW)
            remote(
                image.at[pl.ds(source, length), class_rows(theirs)], part.at[slot, pl.ds(target, length)],
                sum_send.at[0], rs_recv.at[piece], at_shot(offset),
            ).start()

    for rnd in range(rounds):
        for field in range(2):
            both_steps(rnd, field, 3, depth - 2, 4, depth - 4)
        if rnd + 1 == rounds:
            scatter(0, 4, half, 0)
        for side in sides:
            for field in range(2):
                @pl.when(exists(side))
                def _():
                    if rnd == 0:
                        arrived(4 - field, rnd, field, side)
                    else:
                        arrived(2, rnd, field, side)

                both_steps(rnd, field, 1 + depth * side, 2, 2 + (depth - 2) * side, 2)

                if rnd + 1 == rounds and field == 1:
                    scatter(1, 2 + (depth - 2) * side, 2, half + 2 * side)

                @pl.when(exists(side))
                def _():
                    if rnd + 1 < rounds:
                        send_halo(rnd + 1, field, side)
                    elif field == 0:
                        last_u(side)
        if rnd == 0:
            pl.semaphore_wait(near_sem.at[0], 2)
            for offset in (2, -2):
                signal(near_sem.at[1], at_slab(offset))
        elif rnd == 1:
            pl.semaphore_wait(near_sem.at[1], 2)
        if 0 < rnd < 3:
            pl.semaphore_wait(far_sem.at[rnd - 1], 2)
            for offset in (1 << rnd, -(1 << rnd)):
                signal(far_sem.at[rnd], at_shot(offset))

    def at_group(turn):
        return lax.rem(my_group + turn + count, count)

    def passed(piece, turn):
        start = half * piece
        mine = groups_sum.at[my_group, pl.ds(start, half)]
        return remote(
            mine, mine, sum_send.at[1], gs_recv.at[piece, turn], at_shot(WINDOW if turn else -WINDOW)
        )

    def passed_in(piece, turn):
        start = half * piece
        origin = at_group(-1 if turn else 1)
        theirs = groups_sum.at[origin, pl.ds(start, half)]
        return remote(
            theirs, theirs, sum_send.at[1], gs_recv.at[piece, turn], at_shot(WINDOW if turn else -WINDOW)
        )

    def relayed(piece, turn, origin):
        start = half * piece + (half // 2) * (1 - turn)
        theirs = groups_sum.at[origin, pl.ds(start, half // 2)]
        return remote(
            theirs, theirs, sum_send.at[1], relay_recv.at[piece, turn], at_shot(WINDOW if turn else -WINDOW)
        )

    for piece in range(2):
        absorb(part.at[:, pl.ds(half * piece, half)], rs_recv.at[piece])
        for slot in range(half * piece, half * (piece + 1)):
            plane = slot + 4 if piece == 0 else (slot - half + 2 if slot < half + 2 else slot + 2)
            total = image[plane, class_rows(my_class), :]
            for index in range(len(offsets)):
                total = total + part[index, slot]
            groups_sum[my_group, slot] = total
        if piece == 0:
            pl.semaphore_wait(far_sem.at[2], 2)
        for turn in range(2):
            passed(piece, turn).start()

    on_sides(lambda side: arrived(1, rounds, 0, side))

    def prepare(plane, carry):
        state = now.at[rounds, 0]
        center = state[plane, body, :]
        lap_out[plane - 2] = laplace(state, plane, center)
        base_out[plane - 2] = 2.0 * center - mid[rounds, 0, plane, body, :]
        adjoint_out[plane - 2] = now[rounds, 1, plane, body, :]
        model_out[plane - 2] = mod[plane]
        return carry

    lax.fori_loop(2, depth + 2, prepare, 0)
    for piece in range(2):
        for turn in range(2):
            passed_in(piece, turn).wait_recv()
            relayed(piece, turn, at_group(-1 if turn else 1)).start()

    top = jnp.zeros((height, cols), jnp.float32)
    for piece in range(2):
        for turn in range(2):
            relayed(piece, turn, at_group(2)).wait_recv()
        for slot in range(half * piece, half * (piece + 1)):
            total = groups_sum[0, slot]
            for group in range(1, count):
                total = total + groups_sum[group, slot]
            grad[slot, class_rows(my_class), :] = total
            top = jnp.maximum(top, jnp.abs(total))
        if piece == 1:
            mark_top = tops.at[pl.ds(my_class * slabs + slab, 1)]
            tops[my_class * slabs + slab] = jnp.max(top, axis=0, keepdims=True)

            def tell(turn, carry):
                for offset in offsets:
                    remote(
                        mark_top, mark_top, sum_send.at[3], top_recv.at[0], {**at_shot(offset), **at_slab(turn)}
                    ).start()
                return carry

            def tell_here(turn, carry):
                remote(mark_top, mark_top, sum_send.at[3], top_recv.at[0], at_slab(turn)).start()
                return carry

            lax.fori_loop(0, slabs, tell, 0)
            lax.fori_loop(1, slabs, tell_here, 0)
        for offset in offsets:
            mine = grad.at[pl.ds(half * piece, half), class_rows(my_class)]
            remote(mine, mine, sum_send.at[2], ag_recv.at[piece], at_shot(offset)).start()
    for piece in range(2):
        absorb(part.at[:, pl.ds(half * piece, half)], ag_recv.at[piece])
        for slot in range(half * piece, half * (piece + 1)):
            grad_out[slot] = grad[slot]
    others = tops.at[pl.ds(0, WINDOW * slabs - 1)]
    absorb(others, top_recv.at[0])
    top = tops[0]
    for other in range(1, WINDOW * slabs):
        top = jnp.maximum(top, tops[other])
    peak_out[...] = top

    on_sides(lambda side: absorb(inj.at[0:2, 0 : 2 * rounds + 2], halo_send.at[side]))
    absorb(part, sum_send.at[0])
    absorb(groups_sum.at[pl.ds(0, count - 1)], sum_send.at[1])
    absorb(part, sum_send.at[2])
    absorb(others, sum_send.at[3])


def update(shape, grad, top, model, base, lap, adjoint, new_model_hbm, stepped_hbm, adjoint_hbm, fresh_all, step_all, sem):
    depth = shape[0]
    half = depth // 2
    kept = pltpu.make_async_copy(adjoint, adjoint_hbm.at[0], sem.at[0])
    kept.start()
    peak = jnp.max(top[...], axis=1, keepdims=True) + 1e-6
    copies = [kept]
    for slot in range(depth):
        plane = slot + 2 if slot < half else (slot - half if slot < half + 2 else slot)
        fresh = jnp.clip(model[plane] - 0.1 * grad[slot] / peak, 0.05, 0.3)
        fresh_all[plane] = fresh
        step_all[plane] = base[plane] + fresh * lap[plane]
        if slot == half - 1:
            planes = pl.ds(2, half)
        elif slot == half + 1:
            planes = pl.ds(0, 2)
        elif slot == depth - 1:
            planes = pl.ds(depth - 2, 2)
        else:
            continue
        for source, target in ((fresh_all, new_model_hbm), (step_all, stepped_hbm.at[0])):
            copy = pltpu.make_async_copy(source.at[planes], target.at[planes], sem.at[len(copies)])
            copy.start()
            copies.append(copy)
    for copy in copies:
        copy.wait()


def solution(mesh):
    shots, slabs = mesh.shape["shot"], mesh.shape["slab"]

    def per_device(model, fwd_now, fwd_next, adj_now, adj_next, wavelet, misfit, src_index, rec_index):
        shape = model.shape
        depth, rows, cols = shape
        iters, receivers = misfit.shape[1:]
        rounds = iters // 2
        f32 = jnp.float32
        dma = pltpu.SemaphoreType.DMA
        height = rows // WINDOW
        hbm = pl.BlockSpec(memory_space=pl.ANY)
        vmem = pl.BlockSpec(memory_space=pltpu.VMEM)
        whole = jax.ShapeDtypeStruct(shape, f32)
        arguments = (wavelet, misfit, rec_index, model, fwd_now, fwd_next, adj_now, adj_next)
        results = pl.pallas_call(
            functools.partial(kernel, shape, iters, shots, slabs),
            out_shape=(whole, jax.ShapeDtypeStruct((1, cols), f32), whole, whole, whole, whole),
            in_specs=[pl.BlockSpec(memory_space=pltpu.SMEM)] + [hbm] * 8,
            out_specs=(vmem,) * 6,
            scratch_shapes=[
                pltpu.VMEM((rounds + 1, 2, depth + 4, rows + 2 * PAD, cols), f32),
                pltpu.VMEM((rounds + 1, 2, depth + 4, rows + 2 * PAD, cols), f32),
                pltpu.VMEM((depth + 4, rows, cols), f32),
                pltpu.VMEM((2, depth + 4, rows, cols), f32),
                pltpu.VMEM((depth + 4, rows, cols), f32),
                pltpu.VMEM((iters, depth + 4, rows, cols), f32),
                pltpu.VMEM((depth + 4, rows, cols), f32),
                pltpu.VMEM(((depth + 4) * rows, 3 * receivers), jnp.bfloat16),
                pltpu.VMEM((iters, receivers), f32),
                pltpu.VMEM((1, receivers), jnp.int32),
                pltpu.SMEM((1, iters), f32),
                pltpu.VMEM((WINDOW - 1, depth, height, cols), f32),
                pltpu.VMEM((shots // WINDOW, depth, height, cols), f32),
                pltpu.VMEM(shape, f32),
                pltpu.VMEM((WINDOW * slabs, 1, cols), f32),
                dma((5,)),
                dma((2,)),
                dma((2, 2, 2)),
                pltpu.SemaphoreType.REGULAR((3,)),
                pltpu.SemaphoreType.REGULAR((2,)),
                dma((4,)),
                dma((2,)),
                dma((2, 2)),
                dma((2, 2)),
                dma((2,)),
                dma((1,)),
            ],
            compiler_params=pltpu.CompilerParams(
                collective_id=0, has_side_effects=True, vmem_limit_bytes=48 * 1024 * 1024
            ),
            name="reverse_time",
        )(src_index, *(pltpu.with_memory_space_constraint(value, pltpu.HBM) for value in arguments))
        return pl.pallas_call(
            functools.partial(update, shape),
            out_shape=(
                whole, jax.ShapeDtypeStruct(fwd_now.shape, f32), jax.ShapeDtypeStruct(adj_now.shape, f32)
            ),
            in_specs=[vmem] * 6,
            out_specs=(hbm,) * 3,
            scratch_shapes=[pltpu.VMEM(shape, f32), pltpu.VMEM(shape, f32), dma((7,))],
            compiler_params=pltpu.CompilerParams(vmem_limit_bytes=8 * 1024 * 1024),
            name="model_update",
        )(*results)

    field = P(("groups", "shot"), "slab", None, None)
    model_spec = P(("groups", "slab"), None, None)
    return jax.shard_map(
        per_device,
        mesh=mesh,
        in_specs=(
            model_spec, field, field, field, field,
            P(("groups", "shot"), None), P(("groups", "shot"), None, None), P(("groups", "shot")),
            P(("groups", "shot"), None),
        ),
        out_specs=(model_spec, field, field),
        check_vma=False,
    )
```

```python
import functools

import jax
import jax.numpy as jnp
from jax import lax
from jax.experimental import pallas as pl
from jax.experimental.pallas import tpu as pltpu
from jax.sharding import PartitionSpec as P

WINDOW = 8
PAD = 8
MESH = pl.DeviceIdType.MESH


def kernel(
    shape, iters, shots, slabs,
    src_index, wavelet_hbm, misfit_hbm, rec_hbm, model_hbm, un_hbm, ul_hbm, an_hbm, al_hbm,
    grad_out, peak_out, model_out, base_out, lap_out, adjoint_out,
    now, mid, mod, lus, image, inj, src, onehot, misfit, rec, wavelet,
    part, groups_sum, grad, tops,
    load_sem, halo_send, halo_recv, far_sem, near_sem, sum_send, rs_recv, gs_recv, relay_recv, ag_recv, top_recv,
):
    depth, rows, cols = shape
    rounds = iters // 2
    me = lax.axis_index("shot")
    slab = lax.axis_index("slab")
    odd = lax.rem(slab, 2)
    body = pl.ds(PAD, rows)
    own = pl.ds(2, depth)

    def at_shot(offset):
        return {"shot": lax.rem(me + offset + shots, shots)}

    def at_slab(offset):
        return {"slab": lax.rem(slab + offset + slabs, slabs)}

    def signal(sem, device):
        pl.semaphore_signal(sem, inc=1, device_id=device, device_id_type=MESH)

    def remote(source, target, send, recv, device):
        return pltpu.make_async_remote_copy(
            src_ref=source, dst_ref=target, send_sem=send, recv_sem=recv, device_id=device, device_id_type=MESH
        )

    def absorb(ref, sem):
        pltpu.make_async_copy(ref, ref, sem).wait()

    loads = [
        pltpu.make_async_copy(un_hbm.at[0], now.at[0, 0, own, body], load_sem.at[0]),
        pltpu.make_async_copy(ul_hbm.at[0], mid.at[0, 0, own, body], load_sem.at[0]),
        pltpu.make_async_copy(model_hbm, mod.at[own], load_sem.at[0]),
        pltpu.make_async_copy(an_hbm.at[0], now.at[0, 1, own, body], load_sem.at[1]),
        pltpu.make_async_copy(al_hbm.at[0], mid.at[0, 1, own, body], load_sem.at[1]),
        pltpu.make_async_copy(misfit_hbm.at[0], misfit, load_sem.at[2]),
        pltpu.make_async_copy(rec_hbm, rec, load_sem.at[3]),
        pltpu.make_async_copy(wavelet_hbm, wavelet, load_sem.at[4]),
    ]
    for copy in loads:
        copy.start()
    barrier = pltpu.get_barrier_semaphore()
    for offset in (1, -1):
        signal(barrier, at_slab(offset))
        signal(barrier, at_shot(offset))
    pl.semaphore_wait(barrier, 4)

    sides = (1 - odd, odd)

    def exists(side):
        return jnp.where(side == 0, slab > 0, slab < slabs - 1)

    def send(side, source, target, rnd, field):
        remote(
            source, target, halo_send.at[side], halo_recv.at[rnd % 2, field, 1 - side], {"slab": slab + 2 * side - 1}
        ).start()

    def send_halo(rnd, field, side):
        send(
            side,
            now.at[rnd, field, pl.ds(2 + (depth - 2) * side, 2), body],
            now.at[rnd, field, pl.ds((depth + 2) * (1 - side), 2), body],
            rnd, field,
        )

    def edge(side):
        return pl.ds(2 + (depth - 1) * side, 1)

    def ghost(side):
        return pl.ds(1 + (depth + 1) * side, 1)

    def arrived(planes, rnd, field, side):
        absorb(inj.at[0, pl.ds(0, planes)], halo_recv.at[rnd % 2, field, side])

    def on_sides(action):
        for side in sides:
            @pl.when(exists(side))
            def _():
                action(side)

    def first_u(side):
        send_halo(0, 0, side)
        send(side, mid.at[0, 0, edge(side), body], mid.at[0, 0, ghost(1 - side), body], 0, 0)
        send(side, mod.at[edge(side)], mod.at[ghost(1 - side)], 0, 0)

    def first_a(side):
        send_halo(0, 1, side)
        send(side, mid.at[0, 1, edge(side), body], mid.at[0, 1, ghost(1 - side), body], 0, 1)

    def last_u(side):
        send(side, now.at[rounds, 0, edge(side), body], now.at[rounds, 0, ghost(1 - side), body], rounds, 0)

    absorb(inj.at[0:2, 0 : depth + 4], load_sem.at[0])
    on_sides(first_u)
    absorb(inj.at[0:2, 0:depth], load_sem.at[1])
    on_sides(first_a)
    for offset in (1, -1):
        signal(far_sem.at[0], at_shot(offset))
        signal(near_sem.at[0], at_slab(offset))

    strip = jnp.zeros((PAD, cols), jnp.float32)
    plane0 = jnp.zeros((rows, cols), jnp.float32)

    def borders(*refs):
        def clear(plane, carry):
            for ref in refs:
                for field in range(2):
                    ref[field, plane, 0:PAD, :] = strip
                    ref[field, plane, PAD + rows : PAD + rows + PAD, :] = strip
            return carry

        lax.fori_loop(0, depth + 4, clear, 0)

    borders(now.at[0], mid.at[1])
    for side in range(2):
        @pl.when(jnp.logical_not(exists(side)))
        def _():
            for plane in range(2):
                at = (depth + 2) * side + plane
                mod[at] = plane0
                for field in range(2):
                    mid[0, field, at, body, :] = plane0
                    for rnd in range(rounds + 1):
                        now[rnd, field, at, body, :] = plane0

    for copy in loads[-3:]:
        copy.wait()
    line = lax.shift_right_logical(rec[...], 7)
    lane = jnp.bitwise_and(rec[...], cols - 1)
    src_line = lax.shift_right_logical(src_index[0], 7)
    src_lane = jnp.bitwise_and(src_index[0], cols - 1)
    row_id = lax.broadcasted_iota(jnp.int32, (rows, cols), 0)
    col_id = lax.broadcasted_iota(jnp.int32, (rows, cols), 1)

    def mark(plane, carry):
        here = row_id + (slab * depth + plane - 2) * rows
        hit = jnp.where(here == line, 1.0, 0.0).astype(jnp.bfloat16)
        at = pl.ds(pl.multiple_of(plane * rows, rows), rows)
        for copy in range(3):
            onehot[at, copy * cols : (copy + 1) * cols] = hit
        image[plane] = plane0
        src[plane] = jnp.where((here == src_line) & (col_id == src_lane), 1.0, 0.0)
        return carry

    lax.fori_loop(1, depth + 3, mark, 0)
    cell_id = lax.broadcasted_iota(jnp.int32, (cols, cols), 0)

    def place(k, carry):
        value = jnp.where(cell_id == lane, misfit[pl.ds(k, 1), :], 0.0)
        high = value.astype(jnp.bfloat16)
        value = value - high.astype(jnp.float32)
        middle = value.astype(jnp.bfloat16)
        value = value - middle.astype(jnp.float32)
        pieces = jnp.concatenate([high, middle, value.astype(jnp.bfloat16)], axis=1)
        added = lax.dot_general(
            onehot[rows : (depth + 3) * rows, :], pieces, (((1,), (1,)), ((), ())), preferred_element_type=jnp.float32
        )
        inj[k, 1 : depth + 3] = added.reshape(depth + 2, rows, cols)
        return carry

    lax.fori_loop(0, 2, place, 0)

    first_lane = col_id == 0
    last_lane = col_id == cols - 1

    def laplace(ref, plane, center):
        left = jnp.where(first_lane, 0.0, pltpu.roll(center, 1, 1))
        right = jnp.where(last_lane, 0.0, pltpu.roll(center, cols - 1, 1))
        beside = ref[plane + 1, body, :] + ref[plane - 1, body, :]
        beside = beside + (ref[plane, PAD + 1 : PAD + 1 + rows, :] + ref[plane, PAD - 1 : PAD - 1 + rows, :])
        return beside + (left + right) - 6.0 * center

    def advance(field, state, later, target, start, count, k, slot):
        def one(index, carry):
            plane = start + index
            center = state[plane, body, :]
            lap = laplace(state, plane, center)
            fresh = 2.0 * center - later[plane, body, :] + mod[plane] * lap
            if field == 0:
                lus[slot, plane] = lap
                fresh = fresh + wavelet[0, k] * src[plane]
            else:
                image[plane] = image[plane] + center * lus[slot, plane]
                fresh = fresh + inj[k, plane]
            target[plane, body, :] = fresh
            return carry

        lax.fori_loop(0, count, one, 0)

    def both_steps(rnd, field, first_at, first_count, second_at, second_count):
        a, b, c, d = now.at[rnd, field], mid.at[rnd, field], mid.at[rnd + 1, field], now.at[rnd + 1, field]
        advance(field, a, b, c, first_at, first_count, 2 * rnd, 0)
        advance(field, c, a, d, second_at, second_count, 2 * rnd + 1, 1)

    far = jnp.where(odd == 0, WINDOW // 2, -(WINDOW // 2))
    offsets = [far] + [sign * step for step in range(WINDOW // 2 - 1, 0, -1) for sign in (1, -1)]
    height = rows // WINDOW
    my_class = lax.rem(me, WINDOW)
    my_group = lax.div(me, WINDOW)
    count = shots // WINDOW
    half = depth // 2

    def class_rows(which):
        return pl.ds(pl.multiple_of(which * height, height), height)

    def scatter(piece, source, length, target):
        for slot, offset in enumerate(offsets):
            theirs = lax.rem(me + offset + shots, WINDOW)
            remote(
                image.at[pl.ds(source, length), class_rows(theirs)], part.at[slot, pl.ds(target, length)],
                sum_send.at[0], rs_recv.at[piece], at_shot(offset),
            ).start()

    for rnd in range(rounds):
        for field in range(2):
            both_steps(rnd, field, 3, depth - 2, 4, depth - 4)
        if rnd + 1 == rounds:
            scatter(0, 4, half, 0)
        for turn, side in enumerate(sides):
            if turn == 1 and rnd + 1 < rounds:
                borders(now.at[rnd + 1], mid.at[rnd + 2])
                lax.fori_loop(2 * rnd + 2, 2 * rnd + 4, place, 0)
            for field in range(2):
                @pl.when(exists(side))
                def _():
                    if rnd == 0:
                        arrived(4 - field, rnd, field, side)
                    else:
                        arrived(2, rnd, field, side)

                both_steps(rnd, field, 1 + depth * side, 2, 2 + (depth - 2) * side, 2)

                if rnd + 1 == rounds and field == 1:
                    scatter(1, 2 + (depth - 2) * side, 2, half + 2 * side)

                @pl.when(exists(side))
                def _():
                    if rnd + 1 < rounds:
                        send_halo(rnd + 1, field, side)
                    elif field == 0:
                        last_u(side)
        if rnd == 0:
            pl.semaphore_wait(near_sem.at[0], 2)
            for offset in (2, -2):
                signal(near_sem.at[1], at_slab(offset))
        elif rnd == 1:
            pl.semaphore_wait(near_sem.at[1], 2)
        if 0 < rnd < 3:
            pl.semaphore_wait(far_sem.at[rnd - 1], 2)
            for offset in (1 << rnd, -(1 << rnd)):
                signal(far_sem.at[rnd], at_shot(offset))

    def at_group(turn):
        return lax.rem(my_group + turn + count, count)

    def passed(piece, turn):
        start = half * piece
        mine = groups_sum.at[my_group, pl.ds(start, half)]
        return remote(
            mine, mine, sum_send.at[1], gs_recv.at[piece, turn], at_shot(WINDOW if turn else -WINDOW)
        )

    def passed_in(piece, turn):
        theirs = groups_sum.at[at_group(1 - 2 * turn), pl.ds(half * piece, half)]
        return remote(
            theirs, theirs, sum_send.at[1], gs_recv.at[piece, turn], at_shot((2 * turn - 1) * WINDOW)
        )

    def relayed(piece, turn, origin):
        theirs = groups_sum.at[origin, pl.ds(half * piece + (half // 2) * (1 - turn), half // 2)]
        return remote(
            theirs, theirs, sum_send.at[1], relay_recv.at[piece, turn], at_shot((2 * turn - 1) * WINDOW)
        )

    for piece in range(2):
        absorb(part.at[:, pl.ds(half * piece, half)], rs_recv.at[piece])
        for slot in range(half * piece, half * (piece + 1)):
            plane = slot + 4 if piece == 0 else (slot - half + 2 if slot < half + 2 else slot + 2)
            total = image[plane, class_rows(my_class), :]
            for index in range(len(offsets)):
                total = total + part[index, slot]
            groups_sum[my_group, slot] = total
        if piece == 0:
            pl.semaphore_wait(far_sem.at[2], 2)
        for turn in range(2):
            passed(piece, turn).start()

    on_sides(lambda side: arrived(1, rounds, 0, side))

    def prepare(plane, carry):
        state = now.at[rounds, 0]
        center = state[plane, body, :]
        lap_out[plane - 2] = laplace(state, plane, center)
        base_out[plane - 2] = 2.0 * center - mid[rounds, 0, plane, body, :]
        adjoint_out[plane - 2] = now[rounds, 1, plane, body, :]
        model_out[plane - 2] = mod[plane]
        return carry

    borders(now.at[rounds])
    lax.fori_loop(2, depth + 2, prepare, 0)
    early = jnp.where(at_group(-1) < at_group(1), 1, 0)
    for number, turn in enumerate((early, 1 - early)):
        for piece in range(2):
            passed_in(piece, turn).wait_recv()
            relayed(piece, turn, at_group(1 - 2 * turn)).start()

    top = jnp.zeros((height, cols), jnp.float32)
    for piece in range(2):
        for turn in range(2):
            relayed(piece, turn, at_group(2)).wait_recv()
        for slot in range(half * piece, half * (piece + 1)):
            total = groups_sum[0, slot]
            for group in range(1, count):
                total = total + groups_sum[group, slot]
            grad[slot, class_rows(my_class), :] = total
            top = jnp.maximum(top, jnp.abs(total))
        if piece == 1:
            mark_top = tops.at[pl.ds(my_class * slabs + slab, 1)]
            tops[my_class * slabs + slab] = jnp.max(top, axis=0, keepdims=True)

            def tell(turn, carry):
                for offset in offsets:
                    remote(
                        mark_top, mark_top, sum_send.at[3], top_recv.at[0], {**at_shot(offset), **at_slab(turn)}
                    ).start()
                return carry

            def tell_here(turn, carry):
                remote(mark_top, mark_top, sum_send.at[3], top_recv.at[0], at_slab(turn)).start()
                return carry

            lax.fori_loop(0, slabs, tell, 0)
            lax.fori_loop(1, slabs, tell_here, 0)
        for offset in offsets:
            mine = grad.at[pl.ds(half * piece, half), class_rows(my_class)]
            remote(mine, mine, sum_send.at[2], ag_recv.at[piece], at_shot(offset)).start()
    for piece in range(2):
        absorb(part.at[:, pl.ds(half * piece, half)], ag_recv.at[piece])
        for slot in range(half * piece, half * (piece + 1)):
            grad_out[slot] = grad[slot]
    others = tops.at[pl.ds(0, WINDOW * slabs - 1)]
    absorb(others, top_recv.at[0])
    top = tops[0]
    for other in range(1, WINDOW * slabs):
        top = jnp.maximum(top, tops[other])
    peak_out[...] = top

    on_sides(lambda side: absorb(inj.at[0:2, 0 : 2 * rounds + 2], halo_send.at[side]))
    absorb(part, sum_send.at[0])
    absorb(groups_sum.at[pl.ds(0, count - 1)], sum_send.at[1])
    absorb(part, sum_send.at[2])
    absorb(others, sum_send.at[3])


def update(shape, grad, top, model, base, lap, adjoint, new_model_hbm, stepped_hbm, adjoint_hbm, fresh_all, step_all, sem):
    depth = shape[0]
    half = depth // 2
    kept = pltpu.make_async_copy(adjoint, adjoint_hbm.at[0], sem.at[0])
    kept.start()
    peak = jnp.max(top[...], axis=1, keepdims=True) + 1e-6
    copies = [kept]
    for slot in range(depth):
        plane = slot + 2 if slot < half else (slot - half if slot < half + 2 else slot)
        fresh = jnp.clip(model[plane] - 0.1 * grad[slot] / peak, 0.05, 0.3)
        fresh_all[plane] = fresh
        step_all[plane] = base[plane] + fresh * lap[plane]
        if slot == half - 1:
            planes = pl.ds(2, half)
        elif slot == half + 1:
            planes = pl.ds(0, 2)
        elif slot == depth - 1:
            planes = pl.ds(depth - 2, 2)
        else:
            continue
        for source, target in ((fresh_all, new_model_hbm), (step_all, stepped_hbm.at[0])):
            copy = pltpu.make_async_copy(source.at[planes], target.at[planes], sem.at[len(copies)])
            copy.start()
            copies.append(copy)
    for copy in copies:
        copy.wait()


def solution(mesh):
    shots, slabs = mesh.shape["shot"], mesh.shape["slab"]

    def per_device(model, fwd_now, fwd_next, adj_now, adj_next, wavelet, misfit, src_index, rec_index):
        shape = model.shape
        depth, rows, cols = shape
        iters, receivers = misfit.shape[1:]
        rounds = iters // 2
        f32 = jnp.float32
        dma = pltpu.SemaphoreType.DMA
        height = rows // WINDOW
        hbm = pl.BlockSpec(memory_space=pl.ANY)
        vmem = pl.BlockSpec(memory_space=pltpu.VMEM)
        whole = jax.ShapeDtypeStruct(shape, f32)
        arguments = (wavelet, misfit, rec_index, model, fwd_now, fwd_next, adj_now, adj_next)
        results = pl.pallas_call(
            functools.partial(kernel, shape, iters, shots, slabs),
            out_shape=(whole, jax.ShapeDtypeStruct((1, cols), f32), whole, whole, whole, whole),
            in_specs=[pl.BlockSpec(memory_space=pltpu.SMEM)] + [hbm] * 8,
            out_specs=(vmem,) * 6,
            scratch_shapes=[
                pltpu.VMEM((rounds + 1, 2, depth + 4, rows + 2 * PAD, cols), f32),
                pltpu.VMEM((rounds + 1, 2, depth + 4, rows + 2 * PAD, cols), f32),
                pltpu.VMEM((depth + 4, rows, cols), f32),
                pltpu.VMEM((2, depth + 4, rows, cols), f32),
                pltpu.VMEM((depth + 4, rows, cols), f32),
                pltpu.VMEM((iters, depth + 4, rows, cols), f32),
                pltpu.VMEM((depth + 4, rows, cols), f32),
                pltpu.VMEM(((depth + 4) * rows, 3 * receivers), jnp.bfloat16),
                pltpu.VMEM((iters, receivers), f32),
                pltpu.VMEM((1, receivers), jnp.int32),
                pltpu.SMEM((1, iters), f32),
                pltpu.VMEM((WINDOW - 1, depth, height, cols), f32),
                pltpu.VMEM((shots // WINDOW, depth, height, cols), f32),
                pltpu.VMEM(shape, f32),
                pltpu.VMEM((WINDOW * slabs, 1, cols), f32),
                dma((5,)),
                dma((2,)),
                dma((2, 2, 2)),
                pltpu.SemaphoreType.REGULAR((3,)),
                pltpu.SemaphoreType.REGULAR((2,)),
                dma((4,)),
                dma((2,)),
                dma((2, 2)),
                dma((2, 2)),
                dma((2,)),
                dma((1,)),
            ],
            compiler_params=pltpu.CompilerParams(
                collective_id=0, has_side_effects=True, vmem_limit_bytes=48 * 1024 * 1024
            ),
            name="reverse_time",
        )(src_index, *(pltpu.with_memory_space_constraint(value, pltpu.HBM) for value in arguments))
        return pl.pallas_call(
            functools.partial(update, shape),
            out_shape=(
                whole, jax.ShapeDtypeStruct(fwd_now.shape, f32), jax.ShapeDtypeStruct(adj_now.shape, f32)
            ),
            in_specs=[vmem] * 6,
            out_specs=(hbm,) * 3,
            scratch_shapes=[pltpu.VMEM(shape, f32), pltpu.VMEM(shape, f32), dma((7,))],
            compiler_params=pltpu.CompilerParams(vmem_limit_bytes=8 * 1024 * 1024),
            name="model_update",
        )(*results)

    field = P(("groups", "shot"), "slab", None, None)
    model_spec = P(("groups", "slab"), None, None)
    return jax.shard_map(
        per_device,
        mesh=mesh,
        in_specs=(
            model_spec, field, field, field, field,
            P(("groups", "shot"), None), P(("groups", "shot"), None, None), P(("groups", "shot")),
            P(("groups", "shot"), None),
        ),
        out_specs=(model_spec, field, field),
        check_vma=False,
    )
```

```python
import functools

import jax
import jax.numpy as jnp
from jax import lax
from jax.experimental import pallas as pl
from jax.experimental.pallas import tpu as pltpu
from jax.sharding import PartitionSpec as P

WINDOW = 8
PAD = 8
MESH = pl.DeviceIdType.MESH


def kernel(
    shape, iters, shots, slabs,
    src_index, wavelet_hbm, misfit_hbm, rec_hbm, model_hbm, un_hbm, ul_hbm, an_hbm, al_hbm,
    grad_out, peak_out, model_out, base_out, lap_out, adjoint_out,
    now, mid, mod, lus, image, inj, src, onehot, misfit, rec, wavelet,
    part, groups_sum, grad, tops,
    load_sem, halo_send, halo_recv, far_sem, near_sem, sum_send, rs_recv, gs_recv, relay_recv, ag_recv, top_recv,
):
    depth, rows, cols = shape
    rounds = iters // 2
    me = lax.axis_index("shot")
    slab = lax.axis_index("slab")
    odd = lax.rem(slab, 2)
    body = pl.ds(PAD, rows)
    own = pl.ds(2, depth)

    def at_shot(offset):
        return {"shot": lax.rem(me + offset + shots, shots)}

    def at_slab(offset):
        return {"slab": lax.rem(slab + offset + slabs, slabs)}

    def signal(sem, device):
        pl.semaphore_signal(sem, inc=1, device_id=device, device_id_type=MESH)

    def remote(source, target, send, recv, device):
        return pltpu.make_async_remote_copy(
            src_ref=source, dst_ref=target, send_sem=send, recv_sem=recv, device_id=device, device_id_type=MESH
        )

    def absorb(ref, sem):
        pltpu.make_async_copy(ref, ref, sem).wait()

    loads = [
        pltpu.make_async_copy(un_hbm.at[0], now.at[0, 0, own, body], load_sem.at[0]),
        pltpu.make_async_copy(ul_hbm.at[0], mid.at[0, 0, own, body], load_sem.at[0]),
        pltpu.make_async_copy(model_hbm, mod.at[own], load_sem.at[0]),
        pltpu.make_async_copy(an_hbm.at[0], now.at[0, 1, own, body], load_sem.at[1]),
        pltpu.make_async_copy(al_hbm.at[0], mid.at[0, 1, own, body], load_sem.at[1]),
        pltpu.make_async_copy(misfit_hbm.at[0], misfit, load_sem.at[2]),
        pltpu.make_async_copy(rec_hbm, rec, load_sem.at[3]),
        pltpu.make_async_copy(wavelet_hbm, wavelet, load_sem.at[4]),
    ]
    for copy in loads:
        copy.start()
    barrier = pltpu.get_barrier_semaphore()
    for offset in (1, -1):
        signal(barrier, at_slab(offset))
        signal(barrier, at_shot(offset))
    pl.semaphore_wait(barrier, 4)

    sides = (1 - odd, odd)

    def exists(side):
        return jnp.where(side == 0, slab > 0, slab < slabs - 1)

    def send(side, source, target, rnd, field):
        remote(
            source, target, halo_send.at[side], halo_recv.at[rnd % 2, field, 1 - side], {"slab": slab + 2 * side - 1}
        ).start()

    def send_halo(rnd, field, side):
        send(
            side,
            now.at[rnd, field, pl.ds(2 + (depth - 2) * side, 2), body],
            now.at[rnd, field, pl.ds((depth + 2) * (1 - side), 2), body],
            rnd, field,
        )

    def edge(side):
        return pl.ds(2 + (depth - 1) * side, 1)

    def ghost(side):
        return pl.ds(1 + (depth + 1) * side, 1)

    def arrived(planes, rnd, field, side):
        absorb(inj.at[0, pl.ds(0, planes)], halo_recv.at[rnd % 2, field, side])

    def on_sides(action):
        for side in sides:
            @pl.when(exists(side))
            def _():
                action(side)

    def first_u(side):
        send_halo(0, 0, side)
        send(side, mid.at[0, 0, edge(side), body], mid.at[0, 0, ghost(1 - side), body], 0, 0)
        send(side, mod.at[edge(side)], mod.at[ghost(1 - side)], 0, 0)

    def first_a(side):
        send_halo(0, 1, side)
        send(side, mid.at[0, 1, edge(side), body], mid.at[0, 1, ghost(1 - side), body], 0, 1)

    def last_u(side):
        send(side, now.at[rounds, 0, edge(side), body], now.at[rounds, 0, ghost(1 - side), body], rounds, 0)

    absorb(inj.at[0:2, 0 : depth + 4], load_sem.at[0])
    on_sides(first_u)
    absorb(inj.at[0:2, 0:depth], load_sem.at[1])
    on_sides(first_a)
    for offset in (1, -1):
        signal(far_sem.at[0], at_shot(offset))
        signal(near_sem.at[0], at_slab(offset))

    strip = jnp.zeros((PAD, cols), jnp.float32)
    plane0 = jnp.zeros((rows, cols), jnp.float32)

    def borders(*refs):
        def clear(plane, carry):
            for ref in refs:
                for field in range(2):
                    ref[field, plane, 0:PAD, :] = strip
                    ref[field, plane, PAD + rows : PAD + rows + PAD, :] = strip
            return carry

        lax.fori_loop(0, depth + 4, clear, 0)

    borders(now.at[0], mid.at[1])
    for side in range(2):
        @pl.when(jnp.logical_not(exists(side)))
        def _():
            for plane in range(2):
                at = (depth + 2) * side + plane
                mod[at] = plane0
                for field in range(2):
                    mid[0, field, at, body, :] = plane0
                    for rnd in range(rounds + 1):
                        now[rnd, field, at, body, :] = plane0

    for copy in loads[-3:]:
        copy.wait()
    line = lax.shift_right_logical(rec[...], 7)
    lane = jnp.bitwise_and(rec[...], cols - 1)
    src_line = lax.shift_right_logical(src_index[0], 7)
    src_lane = jnp.bitwise_and(src_index[0], cols - 1)
    row_id = lax.broadcasted_iota(jnp.int32, (rows, cols), 0)
    col_id = lax.broadcasted_iota(jnp.int32, (rows, cols), 1)

    def mark(plane, carry):
        here = row_id + (slab * depth + plane - 2) * rows
        hit = jnp.where(here == line, 1.0, 0.0).astype(jnp.bfloat16)
        at = pl.ds(pl.multiple_of(plane * rows, rows), rows)
        for copy in range(3):
            onehot[at, copy * cols : (copy + 1) * cols] = hit
        image[plane] = plane0
        src[plane] = jnp.where((here == src_line) & (col_id == src_lane), 1.0, 0.0)
        return carry

    lax.fori_loop(1, depth + 3, mark, 0, unroll=2)
    cell_id = lax.broadcasted_iota(jnp.int32, (cols, cols), 0)

    def place(k, carry):
        value = jnp.where(cell_id == lane, misfit[pl.ds(k, 1), :], 0.0)
        high = value.astype(jnp.bfloat16)
        value = value - high.astype(jnp.float32)
        middle = value.astype(jnp.bfloat16)
        value = value - middle.astype(jnp.float32)
        pieces = jnp.concatenate([high, middle, value.astype(jnp.bfloat16)], axis=1)
        added = lax.dot_general(
            onehot[rows : (depth + 3) * rows, :], pieces, (((1,), (1,)), ((), ())), preferred_element_type=jnp.float32
        )
        inj[k, 1 : depth + 3] = added.reshape(depth + 2, rows, cols)
        return carry

    lax.fori_loop(0, 2, place, 0, unroll=True)

    first_lane = col_id == 0
    last_lane = col_id == cols - 1

    def laplace(ref, plane, center):
        left = jnp.where(first_lane, 0.0, pltpu.roll(center, 1, 1))
        right = jnp.where(last_lane, 0.0, pltpu.roll(center, cols - 1, 1))
        beside = ref[plane + 1, body, :] + ref[plane - 1, body, :]
        beside = beside + (ref[plane, PAD + 1 : PAD + 1 + rows, :] + ref[plane, PAD - 1 : PAD - 1 + rows, :])
        return beside + (left + right) - 6.0 * center

    def advance(field, state, later, target, start, count, k, slot):
        def one(index):
            plane = start + index
            center = state[plane, body, :]
            lap = laplace(state, plane, center)
            fresh = 2.0 * center - later[plane, body, :] + mod[plane] * lap
            if field == 0:
                lus[slot, plane] = lap
                fresh = fresh + wavelet[0, k] * src[plane]
            else:
                image[plane] = image[plane] + center * lus[slot, plane]
                fresh = fresh + inj[k, plane]
            target[plane, body, :] = fresh

        for index in range(count):
            one(index)

    def both_steps(rnd, field, first_at, first_count, second_at, second_count):
        a, b, c, d = now.at[rnd, field], mid.at[rnd, field], mid.at[rnd + 1, field], now.at[rnd + 1, field]
        advance(field, a, b, c, first_at, first_count, 2 * rnd, 0)
        advance(field, c, a, d, second_at, second_count, 2 * rnd + 1, 1)

    far = jnp.where(odd == 0, WINDOW // 2, -(WINDOW // 2))
    offsets = [far] + [sign * step for step in range(WINDOW // 2 - 1, 0, -1) for sign in (1, -1)]
    height = rows // WINDOW
    my_class = lax.rem(me, WINDOW)
    my_group = lax.div(me, WINDOW)
    count = shots // WINDOW
    half = depth // 2

    def class_rows(which):
        return pl.ds(pl.multiple_of(which * height, height), height)

    def scatter(piece, source, length, target):
        for slot, offset in enumerate(offsets):
            theirs = lax.rem(me + offset + shots, WINDOW)
            remote(
                image.at[pl.ds(source, length), class_rows(theirs)], part.at[slot, pl.ds(target, length)],
                sum_send.at[0], rs_recv.at[piece], at_shot(offset),
            ).start()

    for rnd in range(rounds):
        for field in range(2):
            both_steps(rnd, field, 3, depth - 2, 4, depth - 4)
        if rnd + 1 == rounds:
            scatter(0, 4, half, 0)
        for turn, side in enumerate(sides):
            if turn == 1 and rnd + 1 < rounds:
                borders(now.at[rnd + 1], mid.at[rnd + 2])
                lax.fori_loop(2 * rnd + 2, 2 * rnd + 4, place, 0, unroll=True)
            for field in range(2):
                @pl.when(exists(side))
                def _():
                    if rnd == 0:
                        arrived(4 - field, rnd, field, side)
                    else:
                        arrived(2, rnd, field, side)

                both_steps(rnd, field, 1 + depth * side, 2, 2 + (depth - 2) * side, 2)

                if rnd + 1 == rounds and field == 1:
                    scatter(1, 2 + (depth - 2) * side, 2, half + 2 * side)

                @pl.when(exists(side))
                def _():
                    if rnd + 1 < rounds:
                        send_halo(rnd + 1, field, side)
                    elif field == 0:
                        last_u(side)
        if rnd == 0:
            pl.semaphore_wait(near_sem.at[0], 2)
            for offset in (2, -2):
                signal(near_sem.at[1], at_slab(offset))
        elif rnd == 1:
            pl.semaphore_wait(near_sem.at[1], 2)
        if 0 < rnd < 3:
            pl.semaphore_wait(far_sem.at[rnd - 1], 2)
            for offset in (1 << rnd, -(1 << rnd)):
                signal(far_sem.at[rnd], at_shot(offset))

    def at_group(turn):
        return lax.rem(my_group + turn + count, count)

    def passed(piece, turn):
        start = half * piece
        mine = groups_sum.at[my_group, pl.ds(start, half)]
        return remote(
            mine, mine, sum_send.at[1], gs_recv.at[piece, turn], at_shot(WINDOW if turn else -WINDOW)
        )

    def passed_in(piece, turn):
        theirs = groups_sum.at[at_group(1 - 2 * turn), pl.ds(half * piece, half)]
        return remote(
            theirs, theirs, sum_send.at[1], gs_recv.at[piece, turn], at_shot((2 * turn - 1) * WINDOW)
        )

    def relayed(piece, turn, origin):
        theirs = groups_sum.at[origin, pl.ds(half * piece + (half // 2) * (1 - turn), half // 2)]
        return remote(
            theirs, theirs, sum_send.at[1], relay_recv.at[piece, turn], at_shot((2 * turn - 1) * WINDOW)
        )

    for piece in range(2):
        absorb(part.at[:, pl.ds(half * piece, half)], rs_recv.at[piece])
        for slot in range(half * piece, half * (piece + 1)):
            plane = slot + 4 if piece == 0 else (slot - half + 2 if slot < half + 2 else slot + 2)
            total = image[plane, class_rows(my_class), :]
            for index in range(len(offsets)):
                total = total + part[index, slot]
            groups_sum[my_group, slot] = total
        if piece == 0:
            pl.semaphore_wait(far_sem.at[2], 2)
        for turn in range(2):
            passed(piece, turn).start()

    on_sides(lambda side: arrived(1, rounds, 0, side))

    def prepare(plane, carry):
        state = now.at[rounds, 0]
        center = state[plane, body, :]
        lap_out[plane - 2] = laplace(state, plane, center)
        base_out[plane - 2] = 2.0 * center - mid[rounds, 0, plane, body, :]
        adjoint_out[plane - 2] = now[rounds, 1, plane, body, :]
        model_out[plane - 2] = mod[plane]
        return carry

    borders(now.at[rounds])
    lax.fori_loop(2, depth + 2, prepare, 0, unroll=4)
    early = jnp.where(at_group(-1) < at_group(1), 1, 0)
    for number, turn in enumerate((early, 1 - early)):
        for piece in range(2):
            passed_in(piece, turn).wait_recv()
            relayed(piece, turn, at_group(1 - 2 * turn)).start()

    top = jnp.zeros((height, cols), jnp.float32)
    for piece in range(2):
        for turn in range(2):
            relayed(piece, turn, at_group(2)).wait_recv()
        for slot in range(half * piece, half * (piece + 1)):
            total = groups_sum[0, slot]
            for group in range(1, count):
                total = total + groups_sum[group, slot]
            grad[slot, class_rows(my_class), :] = total
            top = jnp.maximum(top, jnp.abs(total))
        if piece == 1:
            mark_top = tops.at[pl.ds(my_class * slabs + slab, 1)]
            tops[my_class * slabs + slab] = jnp.max(top, axis=0, keepdims=True)

            def tell(turn, carry):
                for offset in offsets:
                    remote(
                        mark_top, mark_top, sum_send.at[3], top_recv.at[0], {**at_shot(offset), **at_slab(turn)}
                    ).start()
                return carry

            def tell_here(turn, carry):
                remote(mark_top, mark_top, sum_send.at[3], top_recv.at[0], at_slab(turn)).start()
                return carry

            lax.fori_loop(0, slabs, tell, 0)
            lax.fori_loop(1, slabs, tell_here, 0)
        for offset in offsets:
            mine = grad.at[pl.ds(half * piece, half), class_rows(my_class)]
            remote(mine, mine, sum_send.at[2], ag_recv.at[piece], at_shot(offset)).start()
    for piece in range(2):
        absorb(part.at[:, pl.ds(half * piece, half)], ag_recv.at[piece])
        for slot in range(half * piece, half * (piece + 1)):
            grad_out[slot] = grad[slot]
    others = tops.at[pl.ds(0, WINDOW * slabs - 1)]
    absorb(others, top_recv.at[0])
    top = tops[0]
    for other in range(1, WINDOW * slabs):
        top = jnp.maximum(top, tops[other])
    peak_out[...] = top

    on_sides(lambda side: absorb(inj.at[0:2, 0 : 2 * rounds + 2], halo_send.at[side]))
    absorb(part, sum_send.at[0])
    absorb(groups_sum.at[pl.ds(0, count - 1)], sum_send.at[1])
    absorb(part, sum_send.at[2])
    absorb(others, sum_send.at[3])


def update(shape, grad, top, model, base, lap, adjoint, new_model_hbm, stepped_hbm, adjoint_hbm, fresh_all, step_all, sem):
    depth = shape[0]
    half = depth // 2
    kept = pltpu.make_async_copy(adjoint, adjoint_hbm.at[0], sem.at[0])
    kept.start()
    peak = jnp.max(top[...], axis=1, keepdims=True) + 1e-6
    copies = [kept]
    for slot in range(depth):
        plane = slot + 2 if slot < half else (slot - half if slot < half + 2 else slot)
        fresh = jnp.clip(model[plane] - 0.1 * grad[slot] / peak, 0.05, 0.3)
        fresh_all[plane] = fresh
        step_all[plane] = base[plane] + fresh * lap[plane]
        if slot == half - 1:
            planes = pl.ds(2, half)
        elif slot == half + 1:
            planes = pl.ds(0, 2)
        elif slot == depth - 1:
            planes = pl.ds(depth - 2, 2)
        else:
            continue
        for source, target in ((fresh_all, new_model_hbm), (step_all, stepped_hbm.at[0])):
            copy = pltpu.make_async_copy(source.at[planes], target.at[planes], sem.at[len(copies)])
            copy.start()
            copies.append(copy)
    for copy in copies:
        copy.wait()


def solution(mesh):
    shots, slabs = mesh.shape["shot"], mesh.shape["slab"]

    def per_device(model, fwd_now, fwd_next, adj_now, adj_next, wavelet, misfit, src_index, rec_index):
        shape = model.shape
        depth, rows, cols = shape
        iters, receivers = misfit.shape[1:]
        rounds = iters // 2
        f32 = jnp.float32
        dma = pltpu.SemaphoreType.DMA
        height = rows // WINDOW
        hbm = pl.BlockSpec(memory_space=pl.ANY)
        vmem = pl.BlockSpec(memory_space=pltpu.VMEM)
        whole = jax.ShapeDtypeStruct(shape, f32)
        arguments = (wavelet, misfit, rec_index, model, fwd_now, fwd_next, adj_now, adj_next)
        results = pl.pallas_call(
            functools.partial(kernel, shape, iters, shots, slabs),
            out_shape=(whole, jax.ShapeDtypeStruct((1, cols), f32), whole, whole, whole, whole),
            in_specs=[pl.BlockSpec(memory_space=pltpu.SMEM)] + [hbm] * 8,
            out_specs=(vmem,) * 6,
            scratch_shapes=[
                pltpu.VMEM((rounds + 1, 2, depth + 4, rows + 2 * PAD, cols), f32),
                pltpu.VMEM((rounds + 1, 2, depth + 4, rows + 2 * PAD, cols), f32),
                pltpu.VMEM((depth + 4, rows, cols), f32),
                pltpu.VMEM((2, depth + 4, rows, cols), f32),
                pltpu.VMEM((depth + 4, rows, cols), f32),
                pltpu.VMEM((iters, depth + 4, rows, cols), f32),
                pltpu.VMEM((depth + 4, rows, cols), f32),
                pltpu.VMEM(((depth + 4) * rows, 3 * receivers), jnp.bfloat16),
                pltpu.VMEM((iters, receivers), f32),
                pltpu.VMEM((1, receivers), jnp.int32),
                pltpu.SMEM((1, iters), f32),
                pltpu.VMEM((WINDOW - 1, depth, height, cols), f32),
                pltpu.VMEM((shots // WINDOW, depth, height, cols), f32),
                pltpu.VMEM(shape, f32),
                pltpu.VMEM((WINDOW * slabs, 1, cols), f32),
                dma((5,)),
                dma((2,)),
                dma((2, 2, 2)),
                pltpu.SemaphoreType.REGULAR((3,)),
                pltpu.SemaphoreType.REGULAR((2,)),
                dma((4,)),
                dma((2,)),
                dma((2, 2)),
                dma((2, 2)),
                dma((2,)),
                dma((1,)),
            ],
            compiler_params=pltpu.CompilerParams(
                collective_id=0, has_side_effects=True, vmem_limit_bytes=48 * 1024 * 1024
            ),
            name="reverse_time",
        )(src_index, *(pltpu.with_memory_space_constraint(value, pltpu.HBM) for value in arguments))
        return pl.pallas_call(
            functools.partial(update, shape),
            out_shape=(
                whole, jax.ShapeDtypeStruct(fwd_now.shape, f32), jax.ShapeDtypeStruct(adj_now.shape, f32)
            ),
            in_specs=[vmem] * 6,
            out_specs=(hbm,) * 3,
            scratch_shapes=[pltpu.VMEM(shape, f32), pltpu.VMEM(shape, f32), dma((7,))],
            compiler_params=pltpu.CompilerParams(vmem_limit_bytes=8 * 1024 * 1024),
            name="model_update",
        )(*results)

    field = P(("groups", "shot"), "slab", None, None)
    model_spec = P(("groups", "slab"), None, None)
    return jax.shard_map(
        per_device,
        mesh=mesh,
        in_specs=(
            model_spec, field, field, field, field,
            P(("groups", "shot"), None), P(("groups", "shot"), None, None), P(("groups", "shot")),
            P(("groups", "shot"), None),
        ),
        out_specs=(model_spec, field, field),
        check_vma=False,
    )
```

```python
import functools

import jax
import jax.numpy as jnp
from jax import lax
from jax.experimental import pallas as pl
from jax.experimental.pallas import tpu as pltpu
from jax.sharding import PartitionSpec as P

WINDOW = 8
PAD = 8
MESH = pl.DeviceIdType.MESH


def kernel(
    shape, iters, shots, slabs,
    src_index, wavelet_hbm, misfit_hbm, rec_hbm, model_hbm, un_hbm, ul_hbm, an_hbm, al_hbm,
    grad_out, peak_out, model_out, base_out, lap_out, adjoint_out,
    now, mid, mod, lus, image, inj, src, onehot, misfit, rec, wavelet,
    part, groups_sum, grad, tops,
    load_sem, halo_send, halo_recv, far_sem, near_sem, sum_send, rs_recv, gs_recv, relay_recv, ag_recv, top_recv,
):
    depth, rows, cols = shape
    rounds = iters // 2
    me = lax.axis_index("shot")
    slab = lax.axis_index("slab")
    odd = lax.rem(slab, 2)
    body = pl.ds(PAD, rows)
    own = pl.ds(2, depth)

    def at_shot(offset):
        return {"shot": lax.rem(me + offset + shots, shots)}

    def at_slab(offset):
        return {"slab": lax.rem(slab + offset + slabs, slabs)}

    def signal(sem, device):
        pl.semaphore_signal(sem, inc=1, device_id=device, device_id_type=MESH)

    def remote(source, target, send, recv, device):
        return pltpu.make_async_remote_copy(
            src_ref=source, dst_ref=target, send_sem=send, recv_sem=recv, device_id=device, device_id_type=MESH
        )

    def absorb(ref, sem):
        pltpu.make_async_copy(ref, ref, sem).wait()

    loads = [
        pltpu.make_async_copy(un_hbm.at[0], now.at[0, 0, own, body], load_sem.at[0]),
        pltpu.make_async_copy(ul_hbm.at[0], mid.at[0, 0, own, body], load_sem.at[0]),
        pltpu.make_async_copy(model_hbm, mod.at[own], load_sem.at[0]),
        pltpu.make_async_copy(an_hbm.at[0], now.at[0, 1, own, body], load_sem.at[1]),
        pltpu.make_async_copy(al_hbm.at[0], mid.at[0, 1, own, body], load_sem.at[1]),
        pltpu.make_async_copy(misfit_hbm.at[0], misfit, load_sem.at[2]),
        pltpu.make_async_copy(rec_hbm, rec, load_sem.at[3]),
        pltpu.make_async_copy(wavelet_hbm, wavelet, load_sem.at[4]),
    ]
    for copy in loads:
        copy.start()
    barrier = pltpu.get_barrier_semaphore()
    for offset in (1, -1):
        signal(barrier, at_slab(offset))
        signal(barrier, at_shot(offset))
    pl.semaphore_wait(barrier, 4)

    sides = (1 - odd, odd)

    def exists(side):
        return jnp.where(side == 0, slab > 0, slab < slabs - 1)

    def send(side, source, target, rnd, field):
        remote(
            source, target, halo_send.at[side], halo_recv.at[rnd % 2, field, 1 - side], {"slab": slab + 2 * side - 1}
        ).start()

    def send_halo(rnd, field, side):
        send(
            side,
            now.at[rnd, field, pl.ds(2 + (depth - 2) * side, 2), body],
            now.at[rnd, field, pl.ds((depth + 2) * (1 - side), 2), body],
            rnd, field,
        )

    def edge(side):
        return pl.ds(2 + (depth - 1) * side, 1)

    def ghost(side):
        return pl.ds(1 + (depth + 1) * side, 1)

    def arrived(planes, rnd, field, side):
        absorb(inj.at[0, pl.ds(0, planes)], halo_recv.at[rnd % 2, field, side])

    def on_sides(action):
        for side in sides:
            @pl.when(exists(side))
            def _():
                action(side)

    def first_u(side):
        send_halo(0, 0, side)
        send(side, mid.at[0, 0, edge(side), body], mid.at[0, 0, ghost(1 - side), body], 0, 0)
        send(side, mod.at[edge(side)], mod.at[ghost(1 - side)], 0, 0)

    def first_a(side):
        send_halo(0, 1, side)
        send(side, mid.at[0, 1, edge(side), body], mid.at[0, 1, ghost(1 - side), body], 0, 1)

    def last_u(side):
        send(side, now.at[rounds, 0, edge(side), body], now.at[rounds, 0, ghost(1 - side), body], rounds, 0)

    absorb(inj.at[0:2, 0 : depth + 4], load_sem.at[0])
    on_sides(first_u)
    absorb(inj.at[0:2, 0:depth], load_sem.at[1])
    on_sides(first_a)
    for offset in (1, -1):
        signal(far_sem.at[0], at_shot(offset))
        signal(near_sem.at[0], at_slab(offset))

    strip = jnp.zeros((PAD, cols), jnp.float32)
    plane0 = jnp.zeros((rows, cols), jnp.float32)

    def borders(*refs):
        def clear(plane, carry):
            for ref in refs:
                for field in range(2):
                    ref[field, plane, 0:PAD, :] = strip
                    ref[field, plane, PAD + rows : PAD + rows + PAD, :] = strip
            return carry

        lax.fori_loop(0, depth + 4, clear, 0)

    borders(now.at[0], mid.at[1])
    for side in range(2):
        @pl.when(jnp.logical_not(exists(side)))
        def _():
            for plane in range(2):
                at = (depth + 2) * side + plane
                mod[at] = plane0
                for field in range(2):
                    mid[0, field, at, body, :] = plane0
                    for rnd in range(rounds + 1):
                        now[rnd, field, at, body, :] = plane0

    for copy in loads[-3:]:
        copy.wait()
    line = lax.shift_right_logical(rec[...], 7)
    lane = jnp.bitwise_and(rec[...], cols - 1)
    src_line = lax.shift_right_logical(src_index[0], 7)
    src_lane = jnp.bitwise_and(src_index[0], cols - 1)
    row_id = lax.broadcasted_iota(jnp.int32, (rows, cols), 0)
    col_id = lax.broadcasted_iota(jnp.int32, (rows, cols), 1)

    def mark(plane, carry):
        here = row_id + (slab * depth + plane - 2) * rows
        hit = jnp.where(here == line, 1.0, 0.0).astype(jnp.bfloat16)
        at = pl.ds(pl.multiple_of(plane * rows, rows), rows)
        for copy in range(3):
            onehot[at, copy * cols : (copy + 1) * cols] = hit
        image[plane] = plane0
        src[plane] = jnp.where((here == src_line) & (col_id == src_lane), 1.0, 0.0)
        return carry

    lax.fori_loop(1, depth + 3, mark, 0, unroll=2)
    cell_id = lax.broadcasted_iota(jnp.int32, (cols, cols), 0)

    def place(k, carry):
        value = jnp.where(cell_id == lane, misfit[pl.ds(k, 1), :], 0.0)
        high = value.astype(jnp.bfloat16)
        value = value - high.astype(jnp.float32)
        middle = value.astype(jnp.bfloat16)
        value = value - middle.astype(jnp.float32)
        pieces = jnp.concatenate([high, middle, value.astype(jnp.bfloat16)], axis=1)
        added = lax.dot_general(
            onehot[rows : (depth + 3) * rows, :], pieces, (((1,), (1,)), ((), ())), preferred_element_type=jnp.float32
        )
        inj[k, 1 : depth + 3] = added.reshape(depth + 2, rows, cols)
        return carry

    lax.fori_loop(0, 2, place, 0, unroll=True)

    first_lane = col_id == 0
    last_lane = col_id == cols - 1

    def laplace(ref, plane, center):
        left = jnp.where(first_lane, 0.0, pltpu.roll(center, 1, 1))
        right = jnp.where(last_lane, 0.0, pltpu.roll(center, cols - 1, 1))
        beside = ref[plane + 1, body, :] + ref[plane - 1, body, :]
        beside = beside + (ref[plane, PAD + 1 : PAD + 1 + rows, :] + ref[plane, PAD - 1 : PAD - 1 + rows, :])
        return beside + (left + right) - 6.0 * center

    def advance(field, state, later, target, start, count, k, slot):
        def one(index):
            plane = start + index
            center = state[plane, body, :]
            lap = laplace(state, plane, center)
            fresh = 2.0 * center - later[plane, body, :] + mod[plane] * lap
            if field == 0:
                lus[slot, plane] = lap
                fresh = fresh + wavelet[0, k] * src[plane]
            else:
                image[plane] = image[plane] + center * lus[slot, plane]
                fresh = fresh + inj[k, plane]
            target[plane, body, :] = fresh

        for index in range(count):
            one(index)

    def both_steps(rnd, field, first_at, first_count, second_at, second_count):
        a, b, c, d = now.at[rnd, field], mid.at[rnd, field], mid.at[rnd + 1, field], now.at[rnd + 1, field]
        advance(field, a, b, c, first_at, first_count, 2 * rnd, 0)
        advance(field, c, a, d, second_at, second_count, 2 * rnd + 1, 1)

    far = jnp.where(odd == 0, WINDOW // 2, -(WINDOW // 2))
    offsets = [far] + [sign * step for step in range(WINDOW // 2 - 1, 0, -1) for sign in (1, -1)]
    height = rows // WINDOW
    my_class = lax.rem(me, WINDOW)
    my_group = lax.div(me, WINDOW)
    count = shots // WINDOW
    half = depth // 2
    pieces = ((0, half, 2), (half, 2, (depth - 2) * sides[0]), (half + 2, 2, (depth - 2) * sides[1]))

    def slots(piece):
        return pl.ds(*pieces[piece][:2])

    def class_rows(which):
        return pl.ds(pl.multiple_of(which * height, height), height)

    def scatter(piece):
        start, length, plane = pieces[piece]
        for slot, offset in enumerate(offsets):
            theirs = lax.rem(me + offset + shots, WINDOW)
            remote(
                image.at[pl.ds(plane + 2, length), class_rows(theirs)], part.at[slot, pl.ds(start, length)],
                sum_send.at[0], rs_recv.at[piece], at_shot(offset),
            ).start()

    for rnd in range(rounds):
        for field in range(2):
            both_steps(rnd, field, 3, depth - 2, 4, depth - 4)
        if rnd + 1 == rounds:
            scatter(0)
        for turn, side in enumerate(sides):
            if turn == 1 and rnd + 1 < rounds:
                borders(now.at[rnd + 1], mid.at[rnd + 2])
                lax.fori_loop(2 * rnd + 2, 2 * rnd + 4, place, 0, unroll=True)
            for field in range(2):
                @pl.when(exists(side))
                def _():
                    if rnd == 0:
                        arrived(4 - field, rnd, field, side)
                    else:
                        arrived(2, rnd, field, side)

                both_steps(rnd, field, 1 + depth * side, 2, 2 + (depth - 2) * side, 2)

                if rnd + 1 == rounds and field == 1:
                    scatter(1 + turn)

                @pl.when(exists(side))
                def _():
                    if rnd + 1 < rounds:
                        send_halo(rnd + 1, field, side)
                    elif field == 0:
                        last_u(side)
        if rnd == 0:
            pl.semaphore_wait(near_sem.at[0], 2)
            for offset in (2, -2):
                signal(near_sem.at[1], at_slab(offset))
        elif rnd == 1:
            pl.semaphore_wait(near_sem.at[1], 2)
        if 0 < rnd < 3:
            pl.semaphore_wait(far_sem.at[rnd - 1], 2)
            for offset in (1 << rnd, -(1 << rnd)):
                signal(far_sem.at[rnd], at_shot(offset))

    def at_group(turn):
        return lax.rem(my_group + turn + count, count)

    def passed(piece, turn):
        mine = groups_sum.at[my_group, slots(piece)]
        return remote(
            mine, mine, sum_send.at[1], gs_recv.at[piece, turn], at_shot(WINDOW if turn else -WINDOW)
        )

    def passed_in(piece, turn):
        theirs = groups_sum.at[at_group(1 - 2 * turn), slots(piece)]
        return remote(
            theirs, theirs, sum_send.at[1], gs_recv.at[piece, turn], at_shot((2 * turn - 1) * WINDOW)
        )

    def relayed(piece, turn, origin):
        start, length, _ = pieces[piece]
        theirs = groups_sum.at[origin, pl.ds(start + (length // 2) * (1 - turn), length // 2)]
        return remote(
            theirs, theirs, sum_send.at[1], relay_recv.at[piece, turn], at_shot((2 * turn - 1) * WINDOW)
        )

    for piece, (start, length, plane) in enumerate(pieces):
        absorb(part.at[:, slots(piece)], rs_recv.at[piece])
        for index in range(length):
            total = image[plane + 2 + index, class_rows(my_class), :]
            for other in range(len(offsets)):
                total = total + part[other, start + index]
            groups_sum[my_group, start + index] = total
        if piece == 0:
            pl.semaphore_wait(far_sem.at[2], 2)
        for turn in range(2):
            passed(piece, turn).start()

    on_sides(lambda side: arrived(1, rounds, 0, side))

    def prepare(plane, carry):
        state = now.at[rounds, 0]
        center = state[plane, body, :]
        lap_out[plane - 2] = laplace(state, plane, center)
        base_out[plane - 2] = 2.0 * center - mid[rounds, 0, plane, body, :]
        adjoint_out[plane - 2] = now[rounds, 1, plane, body, :]
        model_out[plane - 2] = mod[plane]
        return carry

    borders(now.at[rounds])
    lax.fori_loop(2, depth + 2, prepare, 0, unroll=4)
    early = jnp.where(at_group(-1) < at_group(1), 1, 0)
    for number, turn in enumerate((early, 1 - early)):
        for piece in range(len(pieces)):
            passed_in(piece, turn).wait_recv()
            relayed(piece, turn, at_group(1 - 2 * turn)).start()

    mark_top = tops.at[pl.ds(my_class * slabs + slab, 1)]

    def tell(offset, first_slab):
        def one(turn, carry):
            where = {**at_shot(offset), **at_slab(turn)} if first_slab == 0 else at_slab(turn)
            remote(mark_top, mark_top, sum_send.at[3], top_recv.at[0], where).start()
            return carry

        lax.fori_loop(first_slab, slabs, one, 0)

    def share(piece):
        for offset in offsets:
            mine = grad.at[slots(piece), class_rows(my_class)]
            remote(mine, mine, sum_send.at[2], ag_recv.at[piece], at_shot(offset)).start()

    top = jnp.zeros((height, cols), jnp.float32)
    for piece, (start, length, plane) in enumerate(pieces):
        for turn in range(2):
            relayed(piece, turn, at_group(2)).wait_recv()
        for slot in range(start, start + length):
            total = groups_sum[0, slot]
            for group in range(1, count):
                total = total + groups_sum[group, slot]
            grad[slot, class_rows(my_class), :] = total
            top = jnp.maximum(top, jnp.abs(total))
        if piece + 1 < len(pieces):
            share(piece)
    tops[my_class * slabs + slab] = jnp.max(top, axis=0, keepdims=True)
    for number, offset in enumerate(offsets):
        tell(offset, 0)
        if number == 2:
            share(len(pieces) - 1)
    tell(0, 1)
    for piece, (start, length, plane) in enumerate(pieces):
        absorb(part.at[:, slots(piece)], ag_recv.at[piece])
        for index in range(length):
            grad_out[plane + index] = grad[start + index]
    others = tops.at[pl.ds(0, WINDOW * slabs - 1)]
    absorb(others, top_recv.at[0])
    top = tops[0]
    for other in range(1, WINDOW * slabs):
        top = jnp.maximum(top, tops[other])
    peak_out[...] = top

    on_sides(lambda side: absorb(inj.at[0:2, 0 : 2 * rounds + 2], halo_send.at[side]))
    absorb(part, sum_send.at[0])
    absorb(groups_sum.at[pl.ds(0, count - 1)], sum_send.at[1])
    absorb(part, sum_send.at[2])
    absorb(others, sum_send.at[3])


def update(shape, grad, top, model, base, lap, adjoint, new_model_hbm, stepped_hbm, adjoint_hbm, fresh_all, step_all, sem):
    depth = shape[0]
    half = depth // 2
    kept = pltpu.make_async_copy(adjoint, adjoint_hbm.at[0], sem.at[0])
    kept.start()
    peak = jnp.max(top[...], axis=1, keepdims=True) + 1e-6
    copies = [kept]
    for plane in range(depth):
        fresh = jnp.clip(model[plane] - 0.1 * grad[plane] / peak, 0.05, 0.3)
        fresh_all[plane] = fresh
        step_all[plane] = base[plane] + fresh * lap[plane]
        if (plane + 1) % half == 0:
            planes = pl.ds(plane + 1 - half, half)
            for source, target in ((fresh_all, new_model_hbm), (step_all, stepped_hbm.at[0])):
                copy = pltpu.make_async_copy(source.at[planes], target.at[planes], sem.at[len(copies)])
                copy.start()
                copies.append(copy)
    for copy in copies:
        copy.wait()


def solution(mesh):
    shots, slabs = mesh.shape["shot"], mesh.shape["slab"]

    def per_device(model, fwd_now, fwd_next, adj_now, adj_next, wavelet, misfit, src_index, rec_index):
        shape = model.shape
        depth, rows, cols = shape
        iters, receivers = misfit.shape[1:]
        rounds = iters // 2
        f32 = jnp.float32
        dma = pltpu.SemaphoreType.DMA
        height = rows // WINDOW
        hbm = pl.BlockSpec(memory_space=pl.ANY)
        vmem = pl.BlockSpec(memory_space=pltpu.VMEM)
        whole = jax.ShapeDtypeStruct(shape, f32)
        arguments = (wavelet, misfit, rec_index, model, fwd_now, fwd_next, adj_now, adj_next)
        results = pl.pallas_call(
            functools.partial(kernel, shape, iters, shots, slabs),
            out_shape=(whole, jax.ShapeDtypeStruct((1, cols), f32), whole, whole, whole, whole),
            in_specs=[pl.BlockSpec(memory_space=pltpu.SMEM)] + [hbm] * 8,
            out_specs=(vmem,) * 6,
            scratch_shapes=[
                pltpu.VMEM((rounds + 1, 2, depth + 4, rows + 2 * PAD, cols), f32),
                pltpu.VMEM((rounds + 1, 2, depth + 4, rows + 2 * PAD, cols), f32),
                pltpu.VMEM((depth + 4, rows, cols), f32),
                pltpu.VMEM((2, depth + 4, rows, cols), f32),
                pltpu.VMEM((depth + 4, rows, cols), f32),
                pltpu.VMEM((iters, depth + 4, rows, cols), f32),
                pltpu.VMEM((depth + 4, rows, cols), f32),
                pltpu.VMEM(((depth + 4) * rows, 3 * receivers), jnp.bfloat16),
                pltpu.VMEM((iters, receivers), f32),
                pltpu.VMEM((1, receivers), jnp.int32),
                pltpu.SMEM((1, iters), f32),
                pltpu.VMEM((WINDOW - 1, depth, height, cols), f32),
                pltpu.VMEM((shots // WINDOW, depth, height, cols), f32),
                pltpu.VMEM(shape, f32),
                pltpu.VMEM((WINDOW * slabs, 1, cols), f32),
                dma((5,)),
                dma((2,)),
                dma((2, 2, 2)),
                pltpu.SemaphoreType.REGULAR((3,)),
                pltpu.SemaphoreType.REGULAR((2,)),
                dma((4,)),
                dma((3,)),
                dma((3, 2)),
                dma((3, 2)),
                dma((3,)),
                dma((1,)),
            ],
            compiler_params=pltpu.CompilerParams(
                collective_id=0, has_side_effects=True, vmem_limit_bytes=48 * 1024 * 1024
            ),
            name="reverse_time",
        )(src_index, *(pltpu.with_memory_space_constraint(value, pltpu.HBM) for value in arguments))
        return pl.pallas_call(
            functools.partial(update, shape),
            out_shape=(
                whole, jax.ShapeDtypeStruct(fwd_now.shape, f32), jax.ShapeDtypeStruct(adj_now.shape, f32)
            ),
            in_specs=[vmem] * 6,
            out_specs=(hbm,) * 3,
            scratch_shapes=[pltpu.VMEM(shape, f32), pltpu.VMEM(shape, f32), dma((5,))],
            compiler_params=pltpu.CompilerParams(vmem_limit_bytes=8 * 1024 * 1024),
            name="model_update",
        )(*results)

    field = P(("groups", "shot"), "slab", None, None)
    model_spec = P(("groups", "slab"), None, None)
    return jax.shard_map(
        per_device,
        mesh=mesh,
        in_specs=(
            model_spec, field, field, field, field,
            P(("groups", "shot"), None), P(("groups", "shot"), None, None), P(("groups", "shot")),
            P(("groups", "shot"), None),
        ),
        out_specs=(model_spec, field, field),
        check_vma=False,
    )
```

```python
import functools

import jax
import jax.numpy as jnp
from jax import lax
from jax.experimental import pallas as pl
from jax.experimental.pallas import tpu as pltpu
from jax.sharding import PartitionSpec as P

WINDOW = 8
PAD = 8
MESH = pl.DeviceIdType.MESH


def kernel(
    shape, iters, shots, slabs,
    src_index, wavelet_hbm, misfit_hbm, rec_hbm, model_hbm, un_hbm, ul_hbm, an_hbm, al_hbm,
    grad_out, peak_out, model_out, base_out, lap_out, adjoint_out,
    now, mid, mod, lus, image, inj, src, onehot, misfit, rec, wavelet,
    part, groups_sum, grad, tops,
    load_sem, halo_send, halo_recv, far_sem, near_sem, sum_send, rs_recv, gs_recv, relay_recv, ag_recv, top_recv,
):
    depth, rows, cols = shape
    rounds = iters // 2
    me = lax.axis_index("shot")
    slab = lax.axis_index("slab")
    odd = lax.rem(slab, 2)
    body = pl.ds(PAD, rows)
    own = pl.ds(2, depth)

    def at_shot(offset):
        return {"shot": lax.rem(me + offset + shots, shots)}

    def at_slab(offset):
        return {"slab": lax.rem(slab + offset + slabs, slabs)}

    def signal(sem, device):
        pl.semaphore_signal(sem, inc=1, device_id=device, device_id_type=MESH)

    def remote(source, target, send, recv, device):
        return pltpu.make_async_remote_copy(
            src_ref=source, dst_ref=target, send_sem=send, recv_sem=recv, device_id=device, device_id_type=MESH
        )

    def absorb(ref, sem):
        pltpu.make_async_copy(ref, ref, sem).wait()

    loads = [
        pltpu.make_async_copy(un_hbm.at[0], now.at[0, 0, own, body], load_sem.at[0]),
        pltpu.make_async_copy(ul_hbm.at[0], mid.at[0, 0, own, body], load_sem.at[0]),
        pltpu.make_async_copy(model_hbm, mod.at[own], load_sem.at[0]),
        pltpu.make_async_copy(an_hbm.at[0], now.at[0, 1, own, body], load_sem.at[1]),
        pltpu.make_async_copy(al_hbm.at[0], mid.at[0, 1, own, body], load_sem.at[1]),
        pltpu.make_async_copy(misfit_hbm.at[0], misfit, load_sem.at[2]),
        pltpu.make_async_copy(rec_hbm, rec, load_sem.at[3]),
        pltpu.make_async_copy(wavelet_hbm, wavelet, load_sem.at[4]),
    ]
    for copy in loads:
        copy.start()
    barrier = pltpu.get_barrier_semaphore()
    for offset in (1, -1):
        signal(barrier, at_slab(offset))
        signal(barrier, at_shot(offset))
    pl.semaphore_wait(barrier, 4)

    sides = (1 - odd, odd)

    def exists(side):
        return jnp.where(side == 0, slab > 0, slab < slabs - 1)

    def send(side, source, target, rnd, field):
        remote(
            source, target, halo_send.at[side], halo_recv.at[rnd % 2, field, 1 - side], {"slab": slab + 2 * side - 1}
        ).start()

    def send_halo(rnd, field, side):
        send(
            side,
            now.at[rnd, field, pl.ds(2 + (depth - 2) * side, 2), body],
            now.at[rnd, field, pl.ds((depth + 2) * (1 - side), 2), body],
            rnd, field,
        )

    def edge(side):
        return pl.ds(2 + (depth - 1) * side, 1)

    def ghost(side):
        return pl.ds(1 + (depth + 1) * side, 1)

    def arrived(planes, rnd, field, side):
        absorb(inj.at[0, pl.ds(0, planes)], halo_recv.at[rnd % 2, field, side])

    def on_sides(action):
        for side in sides:
            @pl.when(exists(side))
            def _():
                action(side)

    def first_u(side):
        send_halo(0, 0, side)
        send(side, mid.at[0, 0, edge(side), body], mid.at[0, 0, ghost(1 - side), body], 0, 0)
        send(side, mod.at[edge(side)], mod.at[ghost(1 - side)], 0, 0)

    def first_a(side):
        send_halo(0, 1, side)
        send(side, mid.at[0, 1, edge(side), body], mid.at[0, 1, ghost(1 - side), body], 0, 1)

    def last_u(side):
        send(side, now.at[rounds, 0, edge(side), body], now.at[rounds, 0, ghost(1 - side), body], rounds, 0)

    absorb(inj.at[0:2, 0 : depth + 4], load_sem.at[0])
    on_sides(first_u)
    absorb(inj.at[0:2, 0:depth], load_sem.at[1])
    on_sides(first_a)
    for offset in (1, -1):
        signal(far_sem.at[0], at_shot(offset))
        signal(near_sem.at[0], at_slab(offset))

    strip = jnp.zeros((PAD, cols), jnp.float32)
    plane0 = jnp.zeros((rows, cols), jnp.float32)

    def borders(*refs):
        def clear(plane, carry):
            for ref in refs:
                for field in range(2):
                    ref[field, plane, 0:PAD, :] = strip
                    ref[field, plane, PAD + rows : PAD + rows + PAD, :] = strip
            return carry

        lax.fori_loop(0, depth + 4, clear, 0)

    borders(now.at[0], mid.at[1])
    for side in range(2):
        @pl.when(jnp.logical_not(exists(side)))
        def _():
            for plane in range(2):
                at = (depth + 2) * side + plane
                mod[at] = plane0
                for field in range(2):
                    mid[0, field, at, body, :] = plane0
                    for rnd in range(rounds + 1):
                        now[rnd, field, at, body, :] = plane0

    for copy in loads[-3:]:
        copy.wait()
    line = lax.shift_right_logical(rec[...], 7)
    lane = jnp.bitwise_and(rec[...], cols - 1)
    src_line = lax.shift_right_logical(src_index[0], 7)
    src_lane = jnp.bitwise_and(src_index[0], cols - 1)
    row_id = lax.broadcasted_iota(jnp.int32, (rows, cols), 0)
    col_id = lax.broadcasted_iota(jnp.int32, (rows, cols), 1)

    def mark(plane, carry):
        here = row_id + (slab * depth + plane - 2) * rows
        hit = jnp.where(here == line, 1.0, 0.0).astype(jnp.bfloat16)
        at = pl.ds(pl.multiple_of(plane * rows, rows), rows)
        for copy in range(3):
            onehot[at, copy * cols : (copy + 1) * cols] = hit
        image[plane] = plane0
        src[plane] = jnp.where((here == src_line) & (col_id == src_lane), 1.0, 0.0)
        return carry

    lax.fori_loop(1, depth + 3, mark, 0, unroll=2)
    cell_id = lax.broadcasted_iota(jnp.int32, (cols, cols), 0)

    def place(k, carry):
        value = jnp.where(cell_id == lane, misfit[pl.ds(k, 1), :], 0.0)
        high = value.astype(jnp.bfloat16)
        value = value - high.astype(jnp.float32)
        middle = value.astype(jnp.bfloat16)
        value = value - middle.astype(jnp.float32)
        pieces = jnp.concatenate([high, middle, value.astype(jnp.bfloat16)], axis=1)
        added = lax.dot_general(
            onehot[rows : (depth + 3) * rows, :], pieces, (((1,), (1,)), ((), ())), preferred_element_type=jnp.float32
        )
        inj[k, 1 : depth + 3] = added.reshape(depth + 2, rows, cols)
        return carry

    lax.fori_loop(0, 2, place, 0, unroll=True)

    first_lane = col_id == 0
    last_lane = col_id == cols - 1

    def laplace(ref, plane, center):
        left = jnp.where(first_lane, 0.0, pltpu.roll(center, 1, 1))
        right = jnp.where(last_lane, 0.0, pltpu.roll(center, cols - 1, 1))
        beside = ref[plane + 1, body, :] + ref[plane - 1, body, :]
        beside = beside + (ref[plane, PAD + 1 : PAD + 1 + rows, :] + ref[plane, PAD - 1 : PAD - 1 + rows, :])
        return beside + (left + right) - 6.0 * center

    def advance(field, state, later, target, start, count, k, slot):
        def one(index):
            plane = start + index
            center = state[plane, body, :]
            lap = laplace(state, plane, center)
            fresh = 2.0 * center - later[plane, body, :] + mod[plane] * lap
            if field == 0:
                lus[slot, plane] = lap
                fresh = fresh + wavelet[0, k] * src[plane]
            else:
                image[plane] = image[plane] + center * lus[slot, plane]
                fresh = fresh + inj[k, plane]
            target[plane, body, :] = fresh

        for index in range(count):
            one(index)

    def both_steps(rnd, field, first_at, first_count, second_at, second_count):
        a, b, c, d = now.at[rnd, field], mid.at[rnd, field], mid.at[rnd + 1, field], now.at[rnd + 1, field]
        advance(field, a, b, c, first_at, first_count, 2 * rnd, 0)
        advance(field, c, a, d, second_at, second_count, 2 * rnd + 1, 1)

    far = jnp.where(odd == 0, WINDOW // 2, -(WINDOW // 2))
    offsets = [far] + [sign * step for step in range(WINDOW // 2 - 1, 0, -1) for sign in (1, -1)]
    height = rows // WINDOW
    my_class = lax.rem(me, WINDOW)
    my_group = lax.div(me, WINDOW)
    count = shots // WINDOW
    half = depth // 2
    pieces = [(0, half, 2)]
    pieces += [(half + 2 * turn, 2, (depth - 2) * side) for turn, side in enumerate(sides)]

    def slots(piece):
        return pl.ds(*pieces[piece][:2])

    def class_rows(which):
        return pl.ds(pl.multiple_of(which * height, height), height)

    def scatter(piece):
        start, length, plane = pieces[piece]
        for slot, offset in enumerate(offsets):
            theirs = lax.rem(me + offset + shots, WINDOW)
            remote(
                image.at[pl.ds(plane + 2, length), class_rows(theirs)], part.at[slot, pl.ds(start, length)],
                sum_send.at[0], rs_recv.at[piece], at_shot(offset),
            ).start()

    for rnd in range(rounds):
        for field in range(2):
            both_steps(rnd, field, 3, depth - 2, 4, depth - 4)
        if rnd + 1 == rounds:
            scatter(0)
        for turn, side in enumerate(sides):
            if turn == 1 and rnd + 1 < rounds:
                borders(now.at[rnd + 1], mid.at[rnd + 2])
                lax.fori_loop(2 * rnd + 2, 2 * rnd + 4, place, 0, unroll=True)
            for field in range(2):
                @pl.when(exists(side))
                def _():
                    if rnd == 0:
                        arrived(4 - field, rnd, field, side)
                    else:
                        arrived(2, rnd, field, side)

                both_steps(rnd, field, 1 + depth * side, 2, 2 + (depth - 2) * side, 2)

                if rnd + 1 == rounds and field == 1:
                    scatter(1 + turn)

                @pl.when(exists(side))
                def _():
                    if rnd + 1 < rounds:
                        send_halo(rnd + 1, field, side)
                    elif field == 0:
                        last_u(side)
        if rnd == 0:
            pl.semaphore_wait(near_sem.at[0], 2)
            for offset in (2, -2):
                signal(near_sem.at[1], at_slab(offset))
        elif rnd == 1:
            pl.semaphore_wait(near_sem.at[1], 2)
        if 0 < rnd < 3:
            pl.semaphore_wait(far_sem.at[rnd - 1], 2)
            for offset in (1 << rnd, -(1 << rnd)):
                signal(far_sem.at[rnd], at_shot(offset))

    def at_group(turn):
        return lax.rem(my_group + turn + count, count)

    def passed(piece, turn):
        mine = groups_sum.at[my_group, slots(piece)]
        return remote(
            mine, mine, sum_send.at[1], gs_recv.at[piece, turn], at_shot(WINDOW if turn else -WINDOW)
        )

    def passed_in(piece, turn):
        theirs = groups_sum.at[at_group(1 - 2 * turn), slots(piece)]
        return remote(
            theirs, theirs, sum_send.at[1], gs_recv.at[piece, turn], at_shot((2 * turn - 1) * WINDOW)
        )

    def relayed(piece, turn, origin):
        start, length, _ = pieces[piece]
        theirs = groups_sum.at[origin, pl.ds(start + (length // 2) * (1 - turn), length // 2)]
        return remote(
            theirs, theirs, sum_send.at[1], relay_recv.at[piece, turn], at_shot((2 * turn - 1) * WINDOW)
        )

    for piece, (start, length, plane) in enumerate(pieces):
        absorb(part.at[:, slots(piece)], rs_recv.at[piece])
        for index in range(length):
            total = image[plane + 2 + index, class_rows(my_class), :]
            for other in range(len(offsets)):
                total = total + part[other, start + index]
            groups_sum[my_group, start + index] = total
        if piece == 0:
            pl.semaphore_wait(far_sem.at[2], 2)
        for turn in range(2):
            passed(piece, turn).start()

    on_sides(lambda side: arrived(1, rounds, 0, side))

    def prepare(plane, carry):
        state = now.at[rounds, 0]
        center = state[plane, body, :]
        lap_out[plane - 2] = laplace(state, plane, center)
        base_out[plane - 2] = 2.0 * center - mid[rounds, 0, plane, body, :]
        adjoint_out[plane - 2] = now[rounds, 1, plane, body, :]
        model_out[plane - 2] = mod[plane]
        return carry

    borders(now.at[rounds])
    lax.fori_loop(2, depth + 2, prepare, 0, unroll=4)
    early = jnp.where(at_group(-1) < at_group(1), 1, 0)
    for number, turn in enumerate((early, 1 - early)):
        for piece in range(len(pieces)):
            passed_in(piece, turn).wait_recv()
            relayed(piece, turn, at_group(1 - 2 * turn)).start()

    mark_top = tops.at[pl.ds(my_class * slabs + slab, 1)]

    def tell(offset):
        for turn in range(slabs):
            if offset is not None or turn > 0:
                where = {**({} if offset is None else at_shot(offset)), **at_slab(turn)}
                remote(mark_top, mark_top, sum_send.at[3], top_recv.at[0], where).start()

    def share(piece):
        for offset in offsets:
            mine = grad.at[slots(piece), class_rows(my_class)]
            remote(mine, mine, sum_send.at[2], ag_recv.at[piece], at_shot(offset)).start()

    top = jnp.zeros((height, cols), jnp.float32)
    for piece, (start, length, plane) in enumerate(pieces):
        for turn in range(2):
            relayed(piece, turn, at_group(2)).wait_recv()
        for slot in range(start, start + length):
            total = groups_sum[0, slot]
            for group in range(1, count):
                total = total + groups_sum[group, slot]
            grad[slot, class_rows(my_class), :] = total
            top = jnp.maximum(top, jnp.abs(total))
        if piece + 1 < len(pieces):
            share(piece)
    tops[my_class * slabs + slab] = jnp.max(top, axis=0, keepdims=True)
    for number, offset in enumerate(offsets):
        tell(offset)
        if number == 2:
            share(len(pieces) - 1)
    tell(None)
    for piece, (start, length, plane) in enumerate(pieces):
        absorb(part.at[:, slots(piece)], ag_recv.at[piece])
        for index in range(length):
            grad_out[plane + index] = grad[start + index]
    others = tops.at[pl.ds(0, WINDOW * slabs - 1)]
    absorb(others, top_recv.at[0])
    top = tops[0]
    for other in range(1, WINDOW * slabs):
        top = jnp.maximum(top, tops[other])
    peak_out[...] = top

    on_sides(lambda side: absorb(inj.at[0:2, 0 : 2 * rounds + 2], halo_send.at[side]))
    absorb(part, sum_send.at[0])
    absorb(groups_sum.at[pl.ds(0, count - 1)], sum_send.at[1])
    absorb(part, sum_send.at[2])
    absorb(others, sum_send.at[3])


def update(shape, grad, top, model, base, lap, adjoint, new_model_hbm, stepped_hbm, adjoint_hbm, fresh_all, step_all, sem):
    depth = shape[0]
    half = depth // 2
    kept = pltpu.make_async_copy(adjoint, adjoint_hbm.at[0], sem.at[0])
    kept.start()
    peak = jnp.max(top[...], axis=1, keepdims=True) + 1e-6
    copies = [kept]
    for plane in range(depth):
        fresh = jnp.clip(model[plane] - 0.1 * grad[plane] / peak, 0.05, 0.3)
        fresh_all[plane] = fresh
        step_all[plane] = base[plane] + fresh * lap[plane]
        if (plane + 1) % half == 0:
            planes = pl.ds(plane + 1 - half, half)
            for source, target in ((fresh_all, new_model_hbm), (step_all, stepped_hbm.at[0])):
                copy = pltpu.make_async_copy(source.at[planes], target.at[planes], sem.at[len(copies)])
                copy.start()
                copies.append(copy)
    for copy in copies:
        copy.wait()


def solution(mesh):
    shots, slabs = mesh.shape["shot"], mesh.shape["slab"]

    def per_device(model, fwd_now, fwd_next, adj_now, adj_next, wavelet, misfit, src_index, rec_index):
        shape = model.shape
        depth, rows, cols = shape
        iters, receivers = misfit.shape[1:]
        rounds = iters // 2
        f32 = jnp.float32
        dma = pltpu.SemaphoreType.DMA
        height = rows // WINDOW
        hbm = pl.BlockSpec(memory_space=pl.ANY)
        vmem = pl.BlockSpec(memory_space=pltpu.VMEM)
        whole = jax.ShapeDtypeStruct(shape, f32)
        arguments = (wavelet, misfit, rec_index, model, fwd_now, fwd_next, adj_now, adj_next)
        results = pl.pallas_call(
            functools.partial(kernel, shape, iters, shots, slabs),
            out_shape=(whole, jax.ShapeDtypeStruct((1, cols), f32), whole, whole, whole, whole),
            in_specs=[pl.BlockSpec(memory_space=pltpu.SMEM)] + [hbm] * 8,
            out_specs=(vmem,) * 6,
            scratch_shapes=[
                pltpu.VMEM((rounds + 1, 2, depth + 4, rows + 2 * PAD, cols), f32),
                pltpu.VMEM((rounds + 1, 2, depth + 4, rows + 2 * PAD, cols), f32),
                pltpu.VMEM((depth + 4, rows, cols), f32),
                pltpu.VMEM((2, depth + 4, rows, cols), f32),
                pltpu.VMEM((depth + 4, rows, cols), f32),
                pltpu.VMEM((iters, depth + 4, rows, cols), f32),
                pltpu.VMEM((depth + 4, rows, cols), f32),
                pltpu.VMEM(((depth + 4) * rows, 3 * receivers), jnp.bfloat16),
                pltpu.VMEM((iters, receivers), f32),
                pltpu.VMEM((1, receivers), jnp.int32),
                pltpu.SMEM((1, iters), f32),
                pltpu.VMEM((WINDOW - 1, depth, height, cols), f32),
                pltpu.VMEM((shots // WINDOW, depth, height, cols), f32),
                pltpu.VMEM(shape, f32),
                pltpu.VMEM((WINDOW * slabs, 1, cols), f32),
                dma((5,)),
                dma((2,)),
                dma((2, 2, 2)),
                pltpu.SemaphoreType.REGULAR((3,)),
                pltpu.SemaphoreType.REGULAR((2,)),
                dma((4,)),
                dma((depth // 2,)),
                dma((depth // 2, 2)),
                dma((depth // 2, 2)),
                dma((depth // 2,)),
                dma((1,)),
            ],
            compiler_params=pltpu.CompilerParams(
                collective_id=0, has_side_effects=True, vmem_limit_bytes=48 * 1024 * 1024
            ),
            name="reverse_time",
        )(src_index, *(pltpu.with_memory_space_constraint(value, pltpu.HBM) for value in arguments))
        return pl.pallas_call(
            functools.partial(update, shape),
            out_shape=(
                whole, jax.ShapeDtypeStruct(fwd_now.shape, f32), jax.ShapeDtypeStruct(adj_now.shape, f32)
            ),
            in_specs=[vmem] * 6,
            out_specs=(hbm,) * 3,
            scratch_shapes=[pltpu.VMEM(shape, f32), pltpu.VMEM(shape, f32), dma((5,))],
            compiler_params=pltpu.CompilerParams(vmem_limit_bytes=8 * 1024 * 1024),
            name="model_update",
        )(*results)

    field = P(("groups", "shot"), "slab", None, None)
    model_spec = P(("groups", "slab"), None, None)
    return jax.shard_map(
        per_device,
        mesh=mesh,
        in_specs=(
            model_spec, field, field, field, field,
            P(("groups", "shot"), None), P(("groups", "shot"), None, None), P(("groups", "shot")),
            P(("groups", "shot"), None),
        ),
        out_specs=(model_spec, field, field),
        check_vma=False,
    )
```

```python
import functools

import jax
import jax.numpy as jnp
from jax import lax
from jax.experimental import pallas as pl
from jax.experimental.pallas import tpu as pltpu
from jax.sharding import PartitionSpec as P

WINDOW = 8
PAD = 8
MESH = pl.DeviceIdType.MESH


def kernel(
    shape, iters, shots, slabs,
    src_index, wavelet_hbm, misfit_hbm, rec_hbm, model_hbm, un_hbm, ul_hbm, an_hbm, al_hbm,
    grad_out, peak_out, model_out, base_out, lap_out, adjoint_out,
    now, mid, mod, lus, image, inj, src, onehot, misfit, rec, wavelet,
    part, groups_sum, grad, tops,
    load_sem, halo_send, halo_recv, far_sem, near_sem, sum_send, rs_recv, gs_recv, relay_recv, ag_recv, top_recv,
):
    depth, rows, cols = shape
    rounds = iters // 2
    me = lax.axis_index("shot")
    slab = lax.axis_index("slab")
    odd = lax.rem(slab, 2)
    body = pl.ds(PAD, rows)
    own = pl.ds(2, depth)

    def at_shot(offset):
        return {"shot": lax.rem(me + offset + shots, shots)}

    def at_slab(offset):
        return {"slab": lax.rem(slab + offset + slabs, slabs)}

    def signal(sem, device):
        pl.semaphore_signal(sem, inc=1, device_id=device, device_id_type=MESH)

    def remote(source, target, send, recv, device):
        return pltpu.make_async_remote_copy(
            src_ref=source, dst_ref=target, send_sem=send, recv_sem=recv, device_id=device, device_id_type=MESH
        )

    def absorb(ref, sem):
        pltpu.make_async_copy(ref, ref, sem).wait()

    def load(source, target, width, near, rest):
        spans = ((0, width, near), (depth - width, width, near), (width, depth - 2 * width, rest))
        return [
            pltpu.make_async_copy(source.at[pl.ds(start, size)], target(pl.ds(2 + start, size)), load_sem.at[sem])
            for start, size, sem in spans
        ]

    groups = [
        load(un_hbm.at[0], lambda planes: now.at[0, 0, planes, body], 2, 0, 2),
        load(ul_hbm.at[0], lambda planes: mid.at[0, 0, planes, body], 1, 0, 2),
        load(model_hbm, lambda planes: mod.at[planes], 1, 0, 2),
        load(an_hbm.at[0], lambda planes: now.at[0, 1, planes, body], 2, 1, 3),
        load(al_hbm.at[0], lambda planes: mid.at[0, 1, planes, body], 1, 1, 3),
    ]
    small = [
        pltpu.make_async_copy(misfit_hbm.at[0], misfit, load_sem.at[4]),
        pltpu.make_async_copy(rec_hbm, rec, load_sem.at[5]),
        pltpu.make_async_copy(wavelet_hbm, wavelet, load_sem.at[6]),
    ]
    loads = [copy for group in groups for copy in group[:2]] + small + [group[2] for group in groups]
    for copy in loads:
        copy.start()
    barrier = pltpu.get_barrier_semaphore()
    for offset in (1, -1):
        signal(barrier, at_slab(offset))
        signal(barrier, at_shot(offset))
    pl.semaphore_wait(barrier, 4)

    sides = (1 - odd, odd)

    def exists(side):
        return jnp.where(side == 0, slab > 0, slab < slabs - 1)

    def send(side, source, target, rnd, field):
        remote(
            source, target, halo_send.at[side], halo_recv.at[rnd % 2, field, 1 - side], {"slab": slab + 2 * side - 1}
        ).start()

    def send_halo(rnd, field, side):
        send(
            side,
            now.at[rnd, field, pl.ds(2 + (depth - 2) * side, 2), body],
            now.at[rnd, field, pl.ds((depth + 2) * (1 - side), 2), body],
            rnd, field,
        )

    def edge(side):
        return pl.ds(2 + (depth - 1) * side, 1)

    def ghost(side):
        return pl.ds(1 + (depth + 1) * side, 1)

    def arrived(planes, rnd, field, side):
        absorb(inj.at[0, pl.ds(0, planes)], halo_recv.at[rnd % 2, field, side])

    def on_sides(action):
        for side in sides:
            @pl.when(exists(side))
            def _():
                action(side)

    def first_u(side):
        send_halo(0, 0, side)
        send(side, mid.at[0, 0, edge(side), body], mid.at[0, 0, ghost(1 - side), body], 0, 0)
        send(side, mod.at[edge(side)], mod.at[ghost(1 - side)], 0, 0)

    def first_a(side):
        send_halo(0, 1, side)
        send(side, mid.at[0, 1, edge(side), body], mid.at[0, 1, ghost(1 - side), body], 0, 1)

    def last_u(side):
        send(side, now.at[rounds, 0, edge(side), body], now.at[rounds, 0, ghost(1 - side), body], rounds, 0)

    absorb(inj.at[0, 0:8], load_sem.at[0])
    on_sides(first_u)
    absorb(inj.at[0, 0:6], load_sem.at[1])
    on_sides(first_a)
    for offset in (1, -1):
        signal(far_sem.at[0], at_shot(offset))
        signal(near_sem.at[0], at_slab(offset))

    strip = jnp.zeros((PAD, cols), jnp.float32)
    plane0 = jnp.zeros((rows, cols), jnp.float32)

    def borders(*refs):
        def clear(plane, carry):
            for ref in refs:
                for field in range(2):
                    ref[field, plane, 0:PAD, :] = strip
                    ref[field, plane, PAD + rows : PAD + rows + PAD, :] = strip
            return carry

        lax.fori_loop(0, depth + 4, clear, 0)

    borders(now.at[0], mid.at[1])
    for side in range(2):
        @pl.when(jnp.logical_not(exists(side)))
        def _():
            for plane in range(2):
                at = (depth + 2) * side + plane
                mod[at] = plane0
                for field in range(2):
                    mid[0, field, at, body, :] = plane0
                    for rnd in range(rounds + 1):
                        now[rnd, field, at, body, :] = plane0

    for copy in small:
        copy.wait()
    line = lax.shift_right_logical(rec[...], 7)
    lane = jnp.bitwise_and(rec[...], cols - 1)
    src_line = lax.shift_right_logical(src_index[0], 7)
    src_lane = jnp.bitwise_and(src_index[0], cols - 1)
    row_id = lax.broadcasted_iota(jnp.int32, (rows, cols), 0)
    col_id = lax.broadcasted_iota(jnp.int32, (rows, cols), 1)

    def mark(plane, carry):
        here = row_id + (slab * depth + plane - 2) * rows
        hit = jnp.where(here == line, 1.0, 0.0).astype(jnp.bfloat16)
        at = pl.ds(pl.multiple_of(plane * rows, rows), rows)
        for copy in range(3):
            onehot[at, copy * cols : (copy + 1) * cols] = hit
        image[plane] = plane0
        src[plane] = jnp.where((here == src_line) & (col_id == src_lane), 1.0, 0.0)
        return carry

    lax.fori_loop(1, depth + 3, mark, 0, unroll=2)
    cell_id = lax.broadcasted_iota(jnp.int32, (cols, cols), 0)

    def place(k, carry):
        value = jnp.where(cell_id == lane, misfit[pl.ds(k, 1), :], 0.0)
        high = value.astype(jnp.bfloat16)
        value = value - high.astype(jnp.float32)
        middle = value.astype(jnp.bfloat16)
        value = value - middle.astype(jnp.float32)
        pieces = jnp.concatenate([high, middle, value.astype(jnp.bfloat16)], axis=1)
        added = lax.dot_general(
            onehot[rows : (depth + 3) * rows, :], pieces, (((1,), (1,)), ((), ())), preferred_element_type=jnp.float32
        )
        inj[k, 1 : depth + 3] = added.reshape(depth + 2, rows, cols)
        return carry

    lax.fori_loop(0, 2, place, 0, unroll=True)

    absorb(inj.at[0:2, 0:depth], load_sem.at[2])
    absorb(inj.at[0:2, 0 : depth - 3], load_sem.at[3])
    first_lane = col_id == 0
    last_lane = col_id == cols - 1

    def laplace(ref, plane, center):
        left = jnp.where(first_lane, 0.0, pltpu.roll(center, 1, 1))
        right = jnp.where(last_lane, 0.0, pltpu.roll(center, cols - 1, 1))
        beside = ref[plane + 1, body, :] + ref[plane - 1, body, :]
        beside = beside + (ref[plane, PAD + 1 : PAD + 1 + rows, :] + ref[plane, PAD - 1 : PAD - 1 + rows, :])
        return beside + (left + right) - 6.0 * center

    def advance(field, state, later, target, start, count, k, slot):
        def one(index):
            plane = start + index
            center = state[plane, body, :]
            lap = laplace(state, plane, center)
            fresh = 2.0 * center - later[plane, body, :] + mod[plane] * lap
            if field == 0:
                lus[slot, plane] = lap
                fresh = fresh + wavelet[0, k] * src[plane]
            else:
                image[plane] = image[plane] + center * lus[slot, plane]
                fresh = fresh + inj[k, plane]
            target[plane, body, :] = fresh

        for index in range(count):
            one(index)

    def both_steps(rnd, field, first_at, first_count, second_at, second_count):
        a, b, c, d = now.at[rnd, field], mid.at[rnd, field], mid.at[rnd + 1, field], now.at[rnd + 1, field]
        advance(field, a, b, c, first_at, first_count, 2 * rnd, 0)
        advance(field, c, a, d, second_at, second_count, 2 * rnd + 1, 1)

    far = jnp.where(odd == 0, WINDOW // 2, -(WINDOW // 2))
    offsets = [far] + [sign * step for step in range(WINDOW // 2 - 1, 0, -1) for sign in (1, -1)]
    height = rows // WINDOW
    my_class = lax.rem(me, WINDOW)
    my_group = lax.div(me, WINDOW)
    count = shots // WINDOW
    half = depth // 2
    pieces = [(0, half, 2)]
    pieces += [(half + 2 * turn, 2, (depth - 2) * side) for turn, side in enumerate(sides)]

    def slots(piece):
        return pl.ds(*pieces[piece][:2])

    def class_rows(which):
        return pl.ds(pl.multiple_of(which * height, height), height)

    def scatter(piece):
        start, length, plane = pieces[piece]
        for slot, offset in enumerate(offsets):
            theirs = lax.rem(me + offset + shots, WINDOW)
            remote(
                image.at[pl.ds(plane + 2, length), class_rows(theirs)], part.at[slot, pl.ds(start, length)],
                sum_send.at[0], rs_recv.at[piece], at_shot(offset),
            ).start()

    for rnd in range(rounds):
        for field in range(2):
            both_steps(rnd, field, 3, depth - 2, 4, depth - 4)
        if rnd + 1 == rounds:
            scatter(0)
        for turn, side in enumerate(sides):
            if turn == 1 and rnd + 1 < rounds:
                borders(now.at[rnd + 1], mid.at[rnd + 2])
                lax.fori_loop(2 * rnd + 2, 2 * rnd + 4, place, 0, unroll=True)
            for field in range(2):
                @pl.when(exists(side))
                def _():
                    if rnd == 0:
                        arrived(4 - field, rnd, field, side)
                    else:
                        arrived(2, rnd, field, side)

                both_steps(rnd, field, 1 + depth * side, 2, 2 + (depth - 2) * side, 2)

                if rnd + 1 == rounds and field == 1:
                    scatter(1 + turn)

                @pl.when(exists(side))
                def _():
                    if rnd + 1 < rounds:
                        send_halo(rnd + 1, field, side)
                    elif field == 0:
                        last_u(side)
        if rnd == 0:
            pl.semaphore_wait(near_sem.at[0], 2)
            for offset in (2, -2):
                signal(near_sem.at[1], at_slab(offset))
        elif rnd == 1:
            pl.semaphore_wait(near_sem.at[1], 2)
        if 0 < rnd < 3:
            pl.semaphore_wait(far_sem.at[rnd - 1], 2)
            for offset in (1 << rnd, -(1 << rnd)):
                signal(far_sem.at[rnd], at_shot(offset))

    def at_group(turn):
        return lax.rem(my_group + turn + count, count)

    def passed(piece, turn):
        mine = groups_sum.at[my_group, slots(piece)]
        return remote(
            mine, mine, sum_send.at[1], gs_recv.at[piece, turn], at_shot(WINDOW if turn else -WINDOW)
        )

    def passed_in(piece, turn):
        theirs = groups_sum.at[at_group(1 - 2 * turn), slots(piece)]
        return remote(
            theirs, theirs, sum_send.at[1], gs_recv.at[piece, turn], at_shot((2 * turn - 1) * WINDOW)
        )

    def relayed(piece, turn, origin):
        start, length, _ = pieces[piece]
        theirs = groups_sum.at[origin, pl.ds(start + (length // 2) * (1 - turn), length // 2)]
        return remote(
            theirs, theirs, sum_send.at[1], relay_recv.at[piece, turn], at_shot((2 * turn - 1) * WINDOW)
        )

    for piece, (start, length, plane) in enumerate(pieces):
        absorb(part.at[:, slots(piece)], rs_recv.at[piece])
        for index in range(length):
            total = image[plane + 2 + index, class_rows(my_class), :]
            for other in range(len(offsets)):
                total = total + part[other, start + index]
            groups_sum[my_group, start + index] = total
        if piece == 0:
            pl.semaphore_wait(far_sem.at[2], 2)
        for turn in range(2):
            passed(piece, turn).start()

    on_sides(lambda side: arrived(1, rounds, 0, side))

    def prepare(plane, carry):
        state = now.at[rounds, 0]
        center = state[plane, body, :]
        lap_out[plane - 2] = laplace(state, plane, center)
        base_out[plane - 2] = 2.0 * center - mid[rounds, 0, plane, body, :]
        adjoint_out[plane - 2] = now[rounds, 1, plane, body, :]
        model_out[plane - 2] = mod[plane]
        return carry

    borders(now.at[rounds])
    lax.fori_loop(2, depth + 2, prepare, 0, unroll=4)
    early = jnp.where(at_group(-1) < at_group(1), 1, 0)
    for number, turn in enumerate((early, 1 - early)):
        for piece in range(len(pieces)):
            passed_in(piece, turn).wait_recv()
            relayed(piece, turn, at_group(1 - 2 * turn)).start()

    mark_top = tops.at[pl.ds(my_class * slabs + slab, 1)]

    def tell(offset):
        for turn in range(slabs):
            if offset is not None or turn > 0:
                where = {**({} if offset is None else at_shot(offset)), **at_slab(turn)}
                remote(mark_top, mark_top, sum_send.at[3], top_recv.at[0], where).start()

    def share(piece):
        for offset in offsets:
            mine = grad.at[slots(piece), class_rows(my_class)]
            remote(mine, mine, sum_send.at[2], ag_recv.at[piece], at_shot(offset)).start()

    top = jnp.zeros((height, cols), jnp.float32)
    for piece, (start, length, plane) in enumerate(pieces):
        for turn in range(2):
            relayed(piece, turn, at_group(2)).wait_recv()
        for slot in range(start, start + length):
            total = groups_sum[0, slot]
            for group in range(1, count):
                total = total + groups_sum[group, slot]
            grad[slot, class_rows(my_class), :] = total
            top = jnp.maximum(top, jnp.abs(total))
        if piece + 1 < len(pieces):
            share(piece)
    tops[my_class * slabs + slab] = jnp.max(top, axis=0, keepdims=True)
    for number, offset in enumerate(offsets):
        tell(offset)
        if number == 2:
            share(len(pieces) - 1)
    tell(None)
    for piece, (start, length, plane) in enumerate(pieces):
        absorb(part.at[:, slots(piece)], ag_recv.at[piece])
        for index in range(length):
            grad_out[plane + index] = grad[start + index]
    others = tops.at[pl.ds(0, WINDOW * slabs - 1)]
    absorb(others, top_recv.at[0])
    top = tops[0]
    for other in range(1, WINDOW * slabs):
        top = jnp.maximum(top, tops[other])
    peak_out[...] = top

    on_sides(lambda side: absorb(inj.at[0:2, 0 : 2 * rounds + 2], halo_send.at[side]))
    absorb(part, sum_send.at[0])
    absorb(groups_sum.at[pl.ds(0, count - 1)], sum_send.at[1])
    absorb(part, sum_send.at[2])
    absorb(others, sum_send.at[3])


def update(shape, grad, top, model, base, lap, adjoint, new_model_hbm, stepped_hbm, adjoint_hbm, fresh_all, step_all, sem):
    depth = shape[0]
    half = depth // 2
    kept = pltpu.make_async_copy(adjoint, adjoint_hbm.at[0], sem.at[0])
    kept.start()
    peak = jnp.max(top[...], axis=1, keepdims=True) + 1e-6
    copies = [kept]
    for plane in range(depth):
        fresh = jnp.clip(model[plane] - 0.1 * grad[plane] / peak, 0.05, 0.3)
        fresh_all[plane] = fresh
        step_all[plane] = base[plane] + fresh * lap[plane]
        if (plane + 1) % half == 0:
            planes = pl.ds(plane + 1 - half, half)
            for source, target in ((fresh_all, new_model_hbm), (step_all, stepped_hbm.at[0])):
                copy = pltpu.make_async_copy(source.at[planes], target.at[planes], sem.at[len(copies)])
                copy.start()
                copies.append(copy)
    for copy in copies:
        copy.wait()


def solution(mesh):
    shots, slabs = mesh.shape["shot"], mesh.shape["slab"]

    def per_device(model, fwd_now, fwd_next, adj_now, adj_next, wavelet, misfit, src_index, rec_index):
        shape = model.shape
        depth, rows, cols = shape
        iters, receivers = misfit.shape[1:]
        rounds = iters // 2
        f32 = jnp.float32
        dma = pltpu.SemaphoreType.DMA
        height = rows // WINDOW
        hbm = pl.BlockSpec(memory_space=pl.ANY)
        vmem = pl.BlockSpec(memory_space=pltpu.VMEM)
        whole = jax.ShapeDtypeStruct(shape, f32)
        arguments = (wavelet, misfit, rec_index, model, fwd_now, fwd_next, adj_now, adj_next)
        results = pl.pallas_call(
            functools.partial(kernel, shape, iters, shots, slabs),
            out_shape=(whole, jax.ShapeDtypeStruct((1, cols), f32), whole, whole, whole, whole),
            in_specs=[pl.BlockSpec(memory_space=pltpu.SMEM)] + [hbm] * 8,
            out_specs=(vmem,) * 6,
            scratch_shapes=[
                pltpu.VMEM((rounds + 1, 2, depth + 4, rows + 2 * PAD, cols), f32),
                pltpu.VMEM((rounds + 1, 2, depth + 4, rows + 2 * PAD, cols), f32),
                pltpu.VMEM((depth + 4, rows, cols), f32),
                pltpu.VMEM((2, depth + 4, rows, cols), f32),
                pltpu.VMEM((depth + 4, rows, cols), f32),
                pltpu.VMEM((iters, depth + 4, rows, cols), f32),
                pltpu.VMEM((depth + 4, rows, cols), f32),
                pltpu.VMEM(((depth + 4) * rows, 3 * receivers), jnp.bfloat16),
                pltpu.VMEM((iters, receivers), f32),
                pltpu.VMEM((1, receivers), jnp.int32),
                pltpu.SMEM((1, iters), f32),
                pltpu.VMEM((WINDOW - 1, depth, height, cols), f32),
                pltpu.VMEM((shots // WINDOW, depth, height, cols), f32),
                pltpu.VMEM(shape, f32),
                pltpu.VMEM((WINDOW * slabs, 1, cols), f32),
                dma((7,)),
                dma((2,)),
                dma((2, 2, 2)),
                pltpu.SemaphoreType.REGULAR((3,)),
                pltpu.SemaphoreType.REGULAR((2,)),
                dma((4,)),
                dma((depth // 2,)),
                dma((depth // 2, 2)),
                dma((depth // 2, 2)),
                dma((depth // 2,)),
                dma((1,)),
            ],
            compiler_params=pltpu.CompilerParams(
                collective_id=0, has_side_effects=True, vmem_limit_bytes=48 * 1024 * 1024
            ),
            name="reverse_time",
        )(src_index, *(pltpu.with_memory_space_constraint(value, pltpu.HBM) for value in arguments))
        return pl.pallas_call(
            functools.partial(update, shape),
            out_shape=(
                whole, jax.ShapeDtypeStruct(fwd_now.shape, f32), jax.ShapeDtypeStruct(adj_now.shape, f32)
            ),
            in_specs=[vmem] * 6,
            out_specs=(hbm,) * 3,
            scratch_shapes=[pltpu.VMEM(shape, f32), pltpu.VMEM(shape, f32), dma((5,))],
            compiler_params=pltpu.CompilerParams(vmem_limit_bytes=8 * 1024 * 1024),
            name="model_update",
        )(*results)

    field = P(("groups", "shot"), "slab", None, None)
    model_spec = P(("groups", "slab"), None, None)
    return jax.shard_map(
        per_device,
        mesh=mesh,
        in_specs=(
            model_spec, field, field, field, field,
            P(("groups", "shot"), None), P(("groups", "shot"), None, None), P(("groups", "shot")),
            P(("groups", "shot"), None),
        ),
        out_specs=(model_spec, field, field),
        check_vma=False,
    )
```

```python
import functools

import jax
import jax.numpy as jnp
from jax import lax
from jax.experimental import pallas as pl
from jax.experimental.pallas import tpu as pltpu
from jax.sharding import PartitionSpec as P

WINDOW = 8
PAD = 8
MESH = pl.DeviceIdType.MESH


def kernel(
    shape, iters, shots, slabs,
    src_index, wavelet_hbm, misfit_hbm, rec_hbm, model_hbm, un_hbm, ul_hbm, an_hbm, al_hbm,
    grad_out, peak_out, model_out, base_out, lap_out, adjoint_out,
    now, mid, mod, lus, image, inj, src, onehot, misfit, rec, wavelet,
    part, groups_sum, grad, tops,
    load_sem, halo_send, halo_recv, far_sem, near_sem, sum_send, rs_recv, gs_recv, relay_recv, ag_recv, top_recv,
):
    depth, rows, cols = shape
    rounds = iters // 2
    me = lax.axis_index("shot")
    slab = lax.axis_index("slab")
    odd = lax.rem(slab, 2)
    body = pl.ds(PAD, rows)
    own = pl.ds(2, depth)

    def at_shot(offset):
        return {"shot": lax.rem(me + offset + shots, shots)}

    def at_slab(offset):
        return {"slab": lax.rem(slab + offset + slabs, slabs)}

    def signal(sem, device):
        pl.semaphore_signal(sem, inc=1, device_id=device, device_id_type=MESH)

    def remote(source, target, send, recv, device):
        return pltpu.make_async_remote_copy(
            src_ref=source, dst_ref=target, send_sem=send, recv_sem=recv, device_id=device, device_id_type=MESH
        )

    def absorb(ref, sem):
        pltpu.make_async_copy(ref, ref, sem).wait()

    def load(source, target, width, near, rest):
        spans = ((0, width, near), (depth - width, width, near), (width, depth - 2 * width, rest))
        return [
            pltpu.make_async_copy(source.at[pl.ds(start, size)], target(pl.ds(2 + start, size)), load_sem.at[sem])
            for start, size, sem in spans
        ]

    groups = [
        load(un_hbm.at[0], lambda planes: now.at[0, 0, planes, body], 2, 0, 2),
        load(ul_hbm.at[0], lambda planes: mid.at[0, 0, planes, body], 1, 0, 2),
        load(model_hbm, lambda planes: mod.at[planes], 1, 0, 2),
        load(an_hbm.at[0], lambda planes: now.at[0, 1, planes, body], 2, 1, 3),
        load(al_hbm.at[0], lambda planes: mid.at[0, 1, planes, body], 1, 1, 3),
    ]
    small = [
        pltpu.make_async_copy(misfit_hbm.at[0], misfit, load_sem.at[4]),
        pltpu.make_async_copy(rec_hbm, rec, load_sem.at[5]),
        pltpu.make_async_copy(wavelet_hbm, wavelet, load_sem.at[6]),
    ]
    loads = [copy for group in groups for copy in group[:2]] + small + [group[2] for group in groups]
    for copy in loads:
        copy.start()
    barrier = pltpu.get_barrier_semaphore()
    for offset in (1, -1):
        signal(barrier, at_slab(offset))
        signal(barrier, at_shot(offset))
    pl.semaphore_wait(barrier, 4)

    sides = (1 - odd, odd)

    def exists(side):
        return jnp.where(side == 0, slab > 0, slab < slabs - 1)

    def send(side, source, target, rnd, field):
        remote(
            source, target, halo_send.at[side], halo_recv.at[rnd % 2, field, 1 - side], {"slab": slab + 2 * side - 1}
        ).start()

    def send_halo(rnd, field, side):
        send(
            side,
            now.at[rnd, field, pl.ds(2 + (depth - 2) * side, 2), body],
            now.at[rnd, field, pl.ds((depth + 2) * (1 - side), 2), body],
            rnd, field,
        )

    def edge(side):
        return pl.ds(2 + (depth - 1) * side, 1)

    def ghost(side):
        return pl.ds(1 + (depth + 1) * side, 1)

    def arrived(planes, rnd, field, side):
        absorb(inj.at[0, pl.ds(0, planes)], halo_recv.at[rnd % 2, field, side])

    def on_sides(action):
        for side in sides:
            @pl.when(exists(side))
            def _():
                action(side)

    def first_u(side):
        send_halo(0, 0, side)
        send(side, mid.at[0, 0, edge(side), body], mid.at[0, 0, ghost(1 - side), body], 0, 0)
        send(side, mod.at[edge(side)], mod.at[ghost(1 - side)], 0, 0)

    def first_a(side):
        send_halo(0, 1, side)
        send(side, mid.at[0, 1, edge(side), body], mid.at[0, 1, ghost(1 - side), body], 0, 1)

    def last_u(side):
        send(side, now.at[rounds, 0, edge(side), body], now.at[rounds, 0, ghost(1 - side), body], rounds, 0)

    absorb(inj.at[0, 0:8], load_sem.at[0])
    on_sides(first_u)
    absorb(inj.at[0, 0:6], load_sem.at[1])
    on_sides(first_a)
    for offset in (1, -1):
        signal(far_sem.at[0], at_shot(offset))
        signal(near_sem.at[0], at_slab(offset))

    strip = jnp.zeros((PAD, cols), jnp.float32)
    plane0 = jnp.zeros((rows, cols), jnp.float32)

    def borders(*refs):
        def clear(plane, carry):
            for ref in refs:
                for field in range(2):
                    ref[field, plane, 0:PAD, :] = strip
                    ref[field, plane, PAD + rows : PAD + rows + PAD, :] = strip
            return carry

        lax.fori_loop(0, depth + 4, clear, 0)

    borders(now.at[0], mid.at[1])
    for side in range(2):
        @pl.when(jnp.logical_not(exists(side)))
        def _():
            for plane in range(2):
                at = (depth + 2) * side + plane
                mod[at] = plane0
                for field in range(2):
                    mid[0, field, at, body, :] = plane0
                    for rnd in range(rounds + 1):
                        now[rnd, field, at, body, :] = plane0

    for copy in small:
        copy.wait()
    line = lax.shift_right_logical(rec[...], 7)
    lane = jnp.bitwise_and(rec[...], cols - 1)
    src_line = lax.shift_right_logical(src_index[0], 7)
    src_lane = jnp.bitwise_and(src_index[0], cols - 1)
    row_id = lax.broadcasted_iota(jnp.int32, (rows, cols), 0)
    col_id = lax.broadcasted_iota(jnp.int32, (rows, cols), 1)

    def mark(plane, carry):
        here = row_id + (slab * depth + plane - 2) * rows
        hit = jnp.where(here == line, 1.0, 0.0).astype(jnp.bfloat16)
        at = pl.ds(pl.multiple_of(plane * rows, rows), rows)
        for copy in range(3):
            onehot[at, copy * cols : (copy + 1) * cols] = hit
        image[plane] = plane0
        src[plane] = jnp.where((here == src_line) & (col_id == src_lane), 1.0, 0.0)
        return carry

    lax.fori_loop(1, depth + 3, mark, 0, unroll=2)
    cell_id = lax.broadcasted_iota(jnp.int32, (cols, cols), 0)

    def place(k, carry):
        value = jnp.where(cell_id == lane, misfit[pl.ds(k, 1), :], 0.0)
        high = value.astype(jnp.bfloat16)
        value = value - high.astype(jnp.float32)
        middle = value.astype(jnp.bfloat16)
        value = value - middle.astype(jnp.float32)
        pieces = jnp.concatenate([high, middle, value.astype(jnp.bfloat16)], axis=1)
        added = lax.dot_general(
            onehot[rows : (depth + 3) * rows, :], pieces, (((1,), (1,)), ((), ())), preferred_element_type=jnp.float32
        )
        inj[k, 1 : depth + 3] = added.reshape(depth + 2, rows, cols)
        return carry

    lax.fori_loop(0, 2, place, 0, unroll=True)

    absorb(inj.at[0:2, 0:depth], load_sem.at[2])
    absorb(inj.at[0:2, 0 : depth - 3], load_sem.at[3])
    first_lane = col_id == 0
    last_lane = col_id == cols - 1

    def laplace(ref, plane, center):
        left = jnp.where(first_lane, 0.0, pltpu.roll(center, 1, 1))
        right = jnp.where(last_lane, 0.0, pltpu.roll(center, cols - 1, 1))
        beside = ref[plane + 1, body, :] + ref[plane - 1, body, :]
        beside = beside + (ref[plane, PAD + 1 : PAD + 1 + rows, :] + ref[plane, PAD - 1 : PAD - 1 + rows, :])
        return beside + (left + right) - 6.0 * center

    def advance(field, state, later, target, start, count, k, slot):
        def one(index):
            plane = start + index
            center = state[plane, body, :]
            lap = laplace(state, plane, center)
            fresh = 2.0 * center - later[plane, body, :] + mod[plane] * lap
            if field == 0:
                lus[slot, plane] = lap
                fresh = fresh + wavelet[0, k] * src[plane]
            else:
                image[plane] = image[plane] + center * lus[slot, plane]
                fresh = fresh + inj[k, plane]
            target[plane, body, :] = fresh

        for index in range(count):
            one(index)

    def both_steps(rnd, field, first_at, first_count, second_at, second_count):
        a, b, c, d = now.at[rnd, field], mid.at[rnd, field], mid.at[rnd + 1, field], now.at[rnd + 1, field]
        advance(field, a, b, c, first_at, first_count, 2 * rnd, 0)
        advance(field, c, a, d, second_at, second_count, 2 * rnd + 1, 1)

    far = jnp.where(odd == 0, WINDOW // 2, -(WINDOW // 2))
    offsets = [far] + [sign * step for step in range(WINDOW // 2 - 1, 0, -1) for sign in (1, -1)]
    height = rows // WINDOW
    my_class = lax.rem(me, WINDOW)
    my_group = lax.div(me, WINDOW)
    count = shots // WINDOW
    half = depth // 2
    pieces = [(0, half, 2)]
    pieces += [(half + 2 * turn, 2, (depth - 2) * side) for turn, side in enumerate(sides)]

    def slots(piece):
        return pl.ds(*pieces[piece][:2])

    def class_rows(which):
        return pl.ds(pl.multiple_of(which * height, height), height)

    def scatter(piece):
        start, length, plane = pieces[piece]
        for slot, offset in enumerate(offsets):
            theirs = lax.rem(me + offset + shots, WINDOW)
            remote(
                image.at[pl.ds(plane + 2, length), class_rows(theirs)], part.at[slot, pl.ds(start, length)],
                sum_send.at[0], rs_recv.at[piece], at_shot(offset),
            ).start()

    for rnd in range(rounds):
        for field in range(2):
            both_steps(rnd, field, 3, depth - 2, 4, depth - 4)
        if rnd + 1 == rounds:
            scatter(0)
        for turn, side in enumerate(sides):
            if turn == 1 and rnd + 1 < rounds:
                borders(now.at[rnd + 1], mid.at[rnd + 2])
                lax.fori_loop(2 * rnd + 2, 2 * rnd + 4, place, 0, unroll=True)
            for field in range(2):
                @pl.when(exists(side))
                def _():
                    if rnd == 0:
                        arrived(4 - field, rnd, field, side)
                    else:
                        arrived(2, rnd, field, side)

                both_steps(rnd, field, 1 + depth * side, 2, 2 + (depth - 2) * side, 2)

                if rnd + 1 == rounds and field == 1:
                    scatter(1 + turn)

                @pl.when(exists(side))
                def _():
                    if rnd + 1 < rounds:
                        send_halo(rnd + 1, field, side)
                    elif field == 0:
                        last_u(side)
        if rnd == 0:
            pl.semaphore_wait(near_sem.at[0], 2)
            for offset in (2, -2):
                signal(near_sem.at[1], at_slab(offset))
        elif rnd == 1:
            pl.semaphore_wait(near_sem.at[1], 2)
        if 0 < rnd < 3:
            pl.semaphore_wait(far_sem.at[rnd - 1], 2)
            for offset in (1 << rnd, -(1 << rnd)):
                signal(far_sem.at[rnd], at_shot(offset))

    def at_group(turn):
        return lax.rem(my_group + turn + count, count)

    def passed(piece, turn):
        mine = groups_sum.at[my_group, slots(piece)]
        return remote(
            mine, mine, sum_send.at[1], gs_recv.at[piece, turn], at_shot(WINDOW if turn else -WINDOW)
        )

    def passed_in(piece, turn):
        theirs = groups_sum.at[at_group(1 - 2 * turn), slots(piece)]
        return remote(
            theirs, theirs, sum_send.at[1], gs_recv.at[piece, turn], at_shot((2 * turn - 1) * WINDOW)
        )

    def relayed(piece, turn, origin):
        start, length, _ = pieces[piece]
        theirs = groups_sum.at[origin, pl.ds(start + (length // 2) * (1 - turn), length // 2)]
        return remote(
            theirs, theirs, sum_send.at[1], relay_recv.at[piece, turn], at_shot((2 * turn - 1) * WINDOW)
        )

    for piece, (start, length, plane) in enumerate(pieces):
        absorb(part.at[:, slots(piece)], rs_recv.at[piece])
        for index in range(length):
            total = image[plane + 2 + index, class_rows(my_class), :]
            for other in range(len(offsets)):
                total = total + part[other, start + index]
            groups_sum[my_group, start + index] = total
        if piece == 0:
            pl.semaphore_wait(far_sem.at[2], 2)
        for turn in range(2):
            passed(piece, turn).start()

    on_sides(lambda side: arrived(1, rounds, 0, side))

    def prepare(plane, carry):
        state = now.at[rounds, 0]
        center = state[plane, body, :]
        lap_out[plane - 2] = laplace(state, plane, center)
        base_out[plane - 2] = 2.0 * center - mid[rounds, 0, plane, body, :]
        adjoint_out[plane - 2] = now[rounds, 1, plane, body, :]
        model_out[plane - 2] = mod[plane]
        return carry

    borders(now.at[rounds])
    lax.fori_loop(2, depth + 2, prepare, 0, unroll=4)
    early = jnp.where(at_group(-1) < at_group(1), 1, 0)
    for number, turn in enumerate((early, 1 - early)):
        for piece in range(len(pieces)):
            passed_in(piece, turn).wait_recv()
            relayed(piece, turn, at_group(1 - 2 * turn)).start()

    mark_top = tops.at[pl.ds(my_class * slabs + slab, 1)]

    def tell(offset):
        for turn in range(slabs):
            if offset is not None or turn > 0:
                where = {**({} if offset is None else at_shot(offset)), **at_slab(turn)}
                remote(mark_top, mark_top, sum_send.at[3], top_recv.at[0], where).start()

    def share(piece):
        for offset in offsets:
            mine = grad.at[slots(piece), class_rows(my_class)]
            remote(mine, mine, sum_send.at[2], ag_recv.at[piece], at_shot(offset)).start()

    top = jnp.zeros((height, cols), jnp.float32)
    for piece, (start, length, plane) in enumerate(pieces):
        for turn in range(2):
            relayed(piece, turn, at_group(2)).wait_recv()
        for slot in range(start, start + length):
            total = groups_sum[0, slot]
            for group in range(1, count):
                total = total + groups_sum[group, slot]
            grad[slot, class_rows(my_class), :] = total
            top = jnp.maximum(top, jnp.abs(total))
        if piece + 1 < len(pieces):
            share(piece)
    tops[my_class * slabs + slab] = jnp.max(top, axis=0, keepdims=True)
    for number, offset in enumerate(offsets):
        tell(offset)
        if number == 4:
            share(len(pieces) - 1)
    tell(None)
    for piece, (start, length, plane) in enumerate(pieces):
        absorb(part.at[:, slots(piece)], ag_recv.at[piece])
        for index in range(length):
            grad_out[plane + index] = grad[start + index]
    others = tops.at[pl.ds(0, WINDOW * slabs - 1)]
    absorb(others, top_recv.at[0])
    top = tops[0]
    for other in range(1, WINDOW * slabs):
        top = jnp.maximum(top, tops[other])
    peak_out[...] = top

    on_sides(lambda side: absorb(inj.at[0:2, 0 : 2 * rounds + 2], halo_send.at[side]))
    absorb(part, sum_send.at[0])
    absorb(groups_sum.at[pl.ds(0, count - 1)], sum_send.at[1])
    absorb(part, sum_send.at[2])
    absorb(others, sum_send.at[3])


def update(shape, grad, top, model, base, lap, adjoint, new_model_hbm, stepped_hbm, adjoint_hbm, fresh_all, step_all, sem):
    depth = shape[0]
    half = depth // 2
    kept = pltpu.make_async_copy(adjoint, adjoint_hbm.at[0], sem.at[0])
    kept.start()
    peak = jnp.max(top[...], axis=1, keepdims=True) + 1e-6
    copies = [kept]
    for plane in range(depth):
        fresh = jnp.clip(model[plane] - 0.1 * grad[plane] / peak, 0.05, 0.3)
        fresh_all[plane] = fresh
        step_all[plane] = base[plane] + fresh * lap[plane]
        if (plane + 1) % half == 0:
            planes = pl.ds(plane + 1 - half, half)
            for source, target in ((fresh_all, new_model_hbm), (step_all, stepped_hbm.at[0])):
                copy = pltpu.make_async_copy(source.at[planes], target.at[planes], sem.at[len(copies)])
                copy.start()
                copies.append(copy)
    for copy in copies:
        copy.wait()


def solution(mesh):
    shots, slabs = mesh.shape["shot"], mesh.shape["slab"]

    def per_device(model, fwd_now, fwd_next, adj_now, adj_next, wavelet, misfit, src_index, rec_index):
        shape = model.shape
        depth, rows, cols = shape
        iters, receivers = misfit.shape[1:]
        rounds = iters // 2
        f32 = jnp.float32
        dma = pltpu.SemaphoreType.DMA
        height = rows // WINDOW
        hbm = pl.BlockSpec(memory_space=pl.ANY)
        vmem = pl.BlockSpec(memory_space=pltpu.VMEM)
        whole = jax.ShapeDtypeStruct(shape, f32)
        arguments = (wavelet, misfit, rec_index, model, fwd_now, fwd_next, adj_now, adj_next)
        results = pl.pallas_call(
            functools.partial(kernel, shape, iters, shots, slabs),
            out_shape=(whole, jax.ShapeDtypeStruct((1, cols), f32), whole, whole, whole, whole),
            in_specs=[pl.BlockSpec(memory_space=pltpu.SMEM)] + [hbm] * 8,
            out_specs=(vmem,) * 6,
            scratch_shapes=[
                pltpu.VMEM((rounds + 1, 2, depth + 4, rows + 2 * PAD, cols), f32),
                pltpu.VMEM((rounds + 1, 2, depth + 4, rows + 2 * PAD, cols), f32),
                pltpu.VMEM((depth + 4, rows, cols), f32),
                pltpu.VMEM((2, depth + 4, rows, cols), f32),
                pltpu.VMEM((depth + 4, rows, cols), f32),
                pltpu.VMEM((iters, depth + 4, rows, cols), f32),
                pltpu.VMEM((depth + 4, rows, cols), f32),
                pltpu.VMEM(((depth + 4) * rows, 3 * receivers), jnp.bfloat16),
                pltpu.VMEM((iters, receivers), f32),
                pltpu.VMEM((1, receivers), jnp.int32),
                pltpu.SMEM((1, iters), f32),
                pltpu.VMEM((WINDOW - 1, depth, height, cols), f32),
                pltpu.VMEM((shots // WINDOW, depth, height, cols), f32),
                pltpu.VMEM(shape, f32),
                pltpu.VMEM((WINDOW * slabs, 1, cols), f32),
                dma((7,)),
                dma((2,)),
                dma((2, 2, 2)),
                pltpu.SemaphoreType.REGULAR((3,)),
                pltpu.SemaphoreType.REGULAR((2,)),
                dma((4,)),
                dma((depth // 2,)),
                dma((depth // 2, 2)),
                dma((depth // 2, 2)),
                dma((depth // 2,)),
                dma((1,)),
            ],
            compiler_params=pltpu.CompilerParams(
                collective_id=0, has_side_effects=True, vmem_limit_bytes=48 * 1024 * 1024
            ),
            name="reverse_time",
        )(src_index, *(pltpu.with_memory_space_constraint(value, pltpu.HBM) for value in arguments))
        return pl.pallas_call(
            functools.partial(update, shape),
            out_shape=(
                whole, jax.ShapeDtypeStruct(fwd_now.shape, f32), jax.ShapeDtypeStruct(adj_now.shape, f32)
            ),
            in_specs=[vmem] * 6,
            out_specs=(hbm,) * 3,
            scratch_shapes=[pltpu.VMEM(shape, f32), pltpu.VMEM(shape, f32), dma((5,))],
            compiler_params=pltpu.CompilerParams(vmem_limit_bytes=8 * 1024 * 1024),
            name="model_update",
        )(*results)

    field = P(("groups", "shot"), "slab", None, None)
    model_spec = P(("groups", "slab"), None, None)
    return jax.shard_map(
        per_device,
        mesh=mesh,
        in_specs=(
            model_spec, field, field, field, field,
            P(("groups", "shot"), None), P(("groups", "shot"), None, None), P(("groups", "shot")),
            P(("groups", "shot"), None),
        ),
        out_specs=(model_spec, field, field),
        check_vma=False,
    )
```
